32 devices in a mesh: groups: 2 (over x), seq: 16 (over z, y, core).
Axes of the slice: x: 2, y: 2, z: 4, core: 2. Of those that a mesh axis runs over, the one named last changes fastest.
Arguments:
- hidden: bfloat16 [1024, 3072], P(('groups', 'seq')), parts along dimension 0, may hold values from -6 to 6
- queries: bfloat16 [1024, 3072], P(('groups', 'seq')), parts along dimension 0, may hold values from -6 to 6
- key_rows: bfloat16 [1024, 3072], P(('groups', 'seq')), parts along dimension 0, may hold values from -6 to 6
- values: bfloat16 [1024, 3072], P(('groups', 'seq')), parts along dimension 0, may hold values from -12 to 12
- query_gain: float32 [2, 128], replicated, may hold values from 0.6 to 5
- key_gain: float32 [2, 128], replicated, may hold values from 0.6 to 5
- gate_table: bfloat16 [8, 2, 3072], P('groups'), parts along dimension 0, may hold values from -6 to 6
- segment: int32 [1024], P(('groups', 'seq')), parts along dimension 0, may hold values from 0 to 3, as said below
- text_count: int32 [8], P('groups'), parts along dimension 0, may hold values from 1 to 40
Outputs:
- mixed: bfloat16 [1024, 3072], P(('groups', 'seq')), parts along dimension 0
The draws below stay inside these ranges and needn't reach their ends.
There are 2 independent parts, one for each index of `groups`. The reference program is written for one: setup_inputs(seed, part) draws one part's arguments, and reference() takes and returns one part's arrays. A program takes and returns all parts, laid end to end along the dimension named above; an argument that names none is the same for every part. Nothing has to cross between parts.
Inputs may be any that keep to these rules, and one draw needn't show every extreme that they name: `segment`: one device holds at most 10 tokens of one request; in every draw some two requests 2 j and 2 j + 1 get exactly 10 tokens from every device. Tokens of one request may lie anywhere on the devices.
All inputs are finite; a program needn't handle non-finite values.
Results may differ from the reference program's by a relative error of at most 0.012.
The reference program's roundings to bfloat16 on the way (of `query_normed`, `key_normed`, `weights` and `attention`) count: a program that leaves them out, or rounds other values in their place, can miss the bound.
Values may be sent and summed in bfloat16 or wider, within the bound.
A program may use at most 64 MiB of HBM per device.

```python
import math
import jax
import jax.numpy as jnp
from jax import lax

HEADS = 24
HEAD_DIM = 128
D = 3072
TOK_DEV = 32
TOKENS = 512
FINE = 4
CAP = 10
REQS = 4
N_SEQ = 16


def layout(key):
    base_key = jax.random.fold_in(key, 7)
    devices = TOKENS // TOK_DEV
    pair_key, seat_key, bias_key = jax.random.split(base_key, 3)
    full_pair = jax.random.randint(pair_key, (), 0, FINE // 2) * 2
    seat_count = FINE * CAP
    seat_slice = jnp.arange(seat_count, dtype=jnp.int32) // CAP
    forced = seat_slice // 2 * 2 == full_pair
    slice_bias = jax.random.randint(bias_key, (FINE,), 0, 1 << 15)

    def one_device(device_key):
        score_key, order_key = jax.random.split(device_key)
        seat_score = (jax.random.randint(score_key, (seat_count,), 0, 1 << 16) + slice_bias[seat_slice]) * seat_count + jnp.arange(seat_count, dtype=jnp.int32)
        seat_score = jnp.where(forced, -1 - jnp.arange(seat_count, dtype=jnp.int32), seat_score)
        chosen = jnp.argsort(seat_score)[:TOK_DEV]
        token_order = jax.random.permutation(order_key, TOK_DEV)
        return seat_slice[chosen][token_order]
    fine_slice = jax.vmap(one_device)(jax.random.split(seat_key, devices)).reshape(TOKENS)
    segment = fine_slice
    return segment


def drawn(key):
    own_key = jax.random.fold_in(key, 11)
    query_key, key_key = jax.random.split(own_key, 2)
    queries = jnp.clip(jax.random.normal(query_key, (TOKENS, D), jnp.float32), -6.0, 6.0)
    key_data = jnp.clip(jax.random.normal(key_key, (TOKENS, D), jnp.float32), -6.0, 6.0)
    return (queries, key_data)


def draw_segment(key, part):
    return layout(key).astype(jnp.int32)


def draw_queries(key, part):
    return drawn(key)[0].astype(jnp.bfloat16)


def draw_key_rows(key, part):
    return drawn(key)[1].astype(jnp.bfloat16)


def gain_draw(key):
    return jax.random.uniform(key, (2, HEAD_DIM), jnp.float32, 0.6, 1.6)


def draw_query_gain(key, part):
    return gain_draw(jax.random.fold_in(key, 21))


def draw_key_gain(key, part):
    return gain_draw(jax.random.fold_in(key, 23))


def with_ends(values, stream_key, smallest, high):
    longest = values.shape.index(max(values.shape))
    spots = []
    for shift in (0, 1):
        where = [jax.random.randint(jax.random.fold_in(stream_key, axis), (), 0, length) for axis, length in enumerate(values.shape)]
        where[longest] = (where[longest] + shift) % values.shape[longest]
        spots.append(tuple(where))
    return values.at[spots[0]].set(smallest).at[spots[1]].set(high)


def steps_of(stream_key, shape, shards, smallest, top_value):
    def one(dim, parts):
        heights = jax.random.uniform(jax.random.fold_in(jax.random.fold_in(stream_key, 6), dim), (parts,), jnp.float32, smallest / len(shards), top_value / len(shards))
        return jnp.repeat(jnp.exp(heights), shape[dim] // parts).reshape((-1,) + (1,) * (len(shape) - dim - 1))

    loudness = one(*shards[0])
    for cut in shards[1:]:
        loudness = loudness * one(*cut)
    return loudness


def centred(key, shape, deviation, reach, cuts=(), held_as=jnp.bfloat16):
    loudness = steps_of(key, shape, cuts, -0.22, 0.18) if cuts else 1.0
    array = jax.random.normal(key, shape, jnp.float32) * deviation * loudness
    return jnp.minimum(jnp.maximum(array, -reach), reach).astype(held_as)


def setup_inputs(seed: int = 0, part: int = 0) -> dict:
    key_list = jax.random.split(jax.random.key(seed), 10)
    own_keys = jax.random.split(jax.random.fold_in(key_list[9], part), 10)
    hidden = centred(own_keys[0], (TOKENS, D), 1.0, 6.0, ((0, 16),))
    queries = draw_queries(jax.random.fold_in(jax.random.fold_in(key_list[9], part), 71), part)
    key_rows = draw_key_rows(jax.random.fold_in(jax.random.fold_in(key_list[9], part), 71), part)
    values = centred(own_keys[3], (TOKENS, D), 2.0, 12.0, ((0, 16),))
    query_gain = draw_query_gain(jax.random.fold_in(key_list[9], 71), part)
    key_gain = draw_key_gain(jax.random.fold_in(key_list[9], 71), part)
    gate_table = centred(own_keys[6], (REQS, 2, D), 1.0, 6.0)
    segment = draw_segment(jax.random.fold_in(jax.random.fold_in(key_list[9], part), 71), part)
    text_count = with_ends(jax.random.randint(own_keys[8], (REQS,), 1, N_SEQ * CAP // 4 + 1), jax.random.fold_in(own_keys[8], 1), 1, (N_SEQ * CAP // 4 + 1) - 1).astype(jnp.int32)
    return dict(hidden=hidden, queries=queries, key_rows=key_rows, values=values, query_gain=query_gain, key_gain=key_gain, gate_table=gate_table, segment=segment, text_count=text_count)


EPSILON = 1e-06
MASKED = -1e+30

def head_norm(rows_in, gains, stream):
    row_count = rows_in.shape[0]
    per_head = rows_in.astype(jnp.float32).reshape(row_count, -1, HEAD_DIM)
    inverse = lax.rsqrt(lax.optimization_barrier(jnp.mean(per_head * per_head, axis=-1, keepdims=True)) + EPSILON)
    gain_rows = jnp.where((stream == 0)[:, None], gains[0][None, :], gains[1][None, :])
    return (per_head * inverse * gain_rows[:, None, :]).astype(jnp.bfloat16).reshape(row_count, -1)

def attend(query_block, block_segment, key_data, value_data, key_segment):
    scores = jnp.einsum('qhd,khd->hqk', query_block.astype(jnp.float32), key_data.astype(jnp.float32)) * (1.0 / math.sqrt(HEAD_DIM))
    allowed = (block_segment[:, None] == key_segment[None, :])[None, :, :]
    scores = jnp.where(allowed, scores, MASKED)
    largest = lax.optimization_barrier(jnp.max(scores, axis=-1, keepdims=True))
    weights = jnp.exp(scores - largest)
    weights = (weights / lax.optimization_barrier(jnp.sum(weights, axis=-1, keepdims=True))).astype(jnp.bfloat16)
    return jnp.einsum('hqk,khd->qhd', weights.astype(jnp.float32), value_data.astype(jnp.float32)).astype(jnp.bfloat16)

def reference(hidden, queries, key_rows, values, query_gain, key_gain, gate_table, segment, text_count):
    requests = text_count.shape[0]
    seg_hot = (segment[:, None] == jnp.arange(requests, dtype=jnp.int32)[None, :]).astype(jnp.int32)
    position = lax.optimization_barrier(jnp.sum((jnp.cumsum(seg_hot, axis=0) - seg_hot) * seg_hot, axis=1))
    text_limit = lax.optimization_barrier(jnp.sum(seg_hot * text_count[None, :], axis=1))
    stream = (position >= text_limit).astype(jnp.int32)
    query_normed = head_norm(queries, query_gain, stream)
    key_normed = head_norm(key_rows, key_gain, stream)
    fine_slice = segment.astype(jnp.int32)
    fine_hot = (fine_slice[:, None] == jnp.arange(FINE, dtype=jnp.int32)[None, :]).astype(jnp.int32)
    slice_rank = lax.optimization_barrier(jnp.sum((jnp.cumsum(fine_hot, axis=0) - fine_hot) * fine_hot, axis=1))
    slice_width = N_SEQ * CAP
    slot_table = jnp.full((FINE, slice_width), TOKENS, jnp.int32).at[fine_slice, slice_rank].set(jnp.arange(TOKENS, dtype=jnp.int32))
    zero_row = jnp.zeros((1, D), jnp.bfloat16)
    query_padded = jnp.concatenate([query_normed, zero_row], axis=0)
    key_padded = jnp.concatenate([key_normed, zero_row], axis=0)
    value_padded = jnp.concatenate([values, zero_row], axis=0)
    segment_padded = jnp.concatenate([segment, jnp.full((1,), -1, jnp.int32)], axis=0)

    def one_slice(slot_index):
        query_slice = jnp.take(query_padded, slot_index, axis=0).reshape(slice_width, HEADS, HEAD_DIM)
        key_slice = jnp.take(key_padded, slot_index, axis=0).reshape(slice_width, HEADS, HEAD_DIM)
        value_slice = jnp.take(value_padded, slot_index, axis=0).reshape(slice_width, HEADS, HEAD_DIM)
        slot_segment = jnp.take(segment_padded, slot_index, axis=0)
        result = attend(query_slice, slot_segment, key_slice, value_slice, slot_segment)
        return result.reshape(slice_width, D)
    blocks = lax.map(one_slice, slot_table)
    attention = jnp.zeros((TOKENS + 1, D), jnp.bfloat16).at[slot_table.reshape(-1)].set(blocks.reshape(-1, D))[:TOKENS]
    gate_rows = jnp.take(gate_table.reshape(requests * 2, D), segment * 2 + stream, axis=0)
    mixed = hidden.astype(jnp.float32) + gate_rows.astype(jnp.float32) * attention.astype(jnp.float32)
    return mixed.astype(jnp.bfloat16)
```

```python
import functools
import math

import jax
import jax.numpy as jnp
from jax import lax
from jax.experimental import pallas as pl
from jax.experimental.pallas import tpu as pltpu
from jax.sharding import PartitionSpec as P

HEAD_DIM = 128


EPSILON = 1e-06
MASKED = -1e30


def head_norm(rows_in, gains, stream):
    row_count = rows_in.shape[0]
    per_head = rows_in.astype(jnp.float32).reshape(row_count, -1, HEAD_DIM)
    inverse = lax.rsqrt(jnp.mean(per_head * per_head, axis=-1, keepdims=True) + EPSILON)
    gain_rows = jnp.where((stream == 0)[:, None], gains[0][None, :], gains[1][None, :])
    return (per_head * inverse * gain_rows[:, None, :]).astype(jnp.bfloat16).reshape(row_count, -1)


def attend(query_block, block_segment, key_data, value_data, key_segment):
    scores = jnp.einsum(
        "qhd,khd->hqk", query_block, key_data, preferred_element_type=jnp.float32
    ) * (1.0 / math.sqrt(HEAD_DIM))
    allowed = (block_segment[:, None] == key_segment[None, :])[None, :, :]
    scores = jnp.where(allowed, scores, MASKED)
    largest = jnp.max(scores, axis=-1, keepdims=True)
    weights = jnp.exp(scores - largest)
    weights = (weights / jnp.sum(weights, axis=-1, keepdims=True)).astype(jnp.bfloat16)
    return jnp.einsum(
        "hqk,khd->qhd", weights, value_data, preferred_element_type=jnp.float32
    ).astype(jnp.bfloat16)


def per_device(
    hidden, queries, key_rows, values, query_gain, key_gain, gate_table, segment, text_count
):
    tok_rows = hidden.shape[0]
    width_all = hidden.shape[1]
    devices = lax.axis_size("seq")
    requests = text_count.shape[0]
    seg_hot = (segment[:, None] == jnp.arange(requests, dtype=jnp.int32)[None, :]).astype(jnp.int32)
    local_counts = jnp.sum(seg_hot, axis=0)
    all_counts = lax.all_gather(local_counts[None, :], "seq", axis=0, tiled=True)
    lower_rows = (jnp.arange(devices, dtype=jnp.int32) < lax.axis_index("seq")).astype(jnp.int32)
    before = jnp.sum(all_counts * lower_rows[:, None], axis=0)
    position = jnp.sum((jnp.cumsum(seg_hot, axis=0) - seg_hot + before[None, :]) * seg_hot, axis=1)
    text_limit = jnp.sum(seg_hot * text_count[None, :], axis=1)
    stream = (position >= text_limit).astype(jnp.int32)
    query_normed = head_norm(queries, query_gain, stream)
    key_normed = head_norm(key_rows, key_gain, stream)
    groups = 8
    pair_merge = 2
    slices = devices // groups
    cap_rows = 4 * tok_rows // devices + max(1, tok_rows // devices)
    bucket_rows = cap_rows * pair_merge
    head_cols = width_all // groups
    owner_slice = segment // pair_merge
    owner_hot = (owner_slice[:, None] == jnp.arange(slices, dtype=jnp.int32)[None, :]).astype(
        jnp.int32
    )
    owner_rank = jnp.sum((jnp.cumsum(owner_hot, axis=0) - owner_hot) * owner_hot, axis=1)
    slot_place = owner_slice * bucket_rows + owner_rank
    bucket_index = (
        jnp.full((slices * bucket_rows,), tok_rows, jnp.int32)
        .at[slot_place]
        .set(jnp.arange(tok_rows, dtype=jnp.int32))
    )
    stacked = jnp.concatenate(
        [
            query_normed.reshape(tok_rows, groups, head_cols),
            key_normed.reshape(tok_rows, groups, head_cols),
            values.reshape(tok_rows, groups, head_cols),
        ],
        axis=2,
    ).transpose(1, 0, 2)
    outgoing = jnp.take(stacked, bucket_index, axis=1, mode="fill", fill_value=0).reshape(
        devices, bucket_rows, 3 * head_cols
    )
    slot_segment = jnp.take(segment, bucket_index, axis=0, mode="fill", fill_value=-1)
    segment_out = jnp.broadcast_to(slot_segment[None, :], (groups, slices * bucket_rows)).reshape(
        devices, bucket_rows
    )
    arrived, arrived_segment = (
        lax.all_to_all(outgoing, "seq", split_axis=0, concat_axis=0, tiled=True),
        lax.all_to_all(segment_out, "seq", split_axis=0, concat_axis=0, tiled=True),
    )
    slot_count = devices * bucket_rows
    per_head = head_cols // HEAD_DIM
    slot_data = arrived.reshape(slot_count, 3 * head_cols)
    query_all = slot_data[:, :head_cols].reshape(slot_count, per_head, HEAD_DIM)
    key_all = slot_data[:, head_cols : 2 * head_cols].reshape(slot_count, per_head, HEAD_DIM)
    value_all = slot_data[:, 2 * head_cols :].reshape(slot_count, per_head, HEAD_DIM)
    key_segment = arrived_segment.reshape(slot_count)
    if slot_count % 512 == 0:
        block_rows = 512
    elif slot_count % 256 == 0:
        block_rows = 256
    else:
        block_rows = slot_count

    def one_block(first_row):
        return attend(query_all, key_segment, key_all, value_all, key_segment)

    results = lax.map(one_block, jnp.arange(slot_count // block_rows, dtype=jnp.int32) * block_rows)
    returning = results.reshape(devices, bucket_rows, head_cols)
    returned = lax.all_to_all(returning, "seq", split_axis=0, concat_axis=0, tiled=True)
    returned = returned.reshape(groups, slices * bucket_rows, head_cols)
    attention = (
        jnp.take(returned, slot_place, axis=1).transpose(1, 0, 2).reshape(tok_rows, width_all)
    )
    gate_rows = jnp.take(gate_table.reshape(requests * 2, width_all), segment * 2 + stream, axis=0)
    mixed = hidden.astype(jnp.float32) + gate_rows.astype(jnp.float32) * attention.astype(
        jnp.float32
    )
    return mixed.astype(jnp.bfloat16)


LANES = 128
CONTRACT_LAST = (((1,), (1,)), ((), ()))


def normed(rows, gain_rows):
    wide = rows.astype(jnp.float32)
    inverse = lax.rsqrt(jnp.mean(wide * wide, axis=-1, keepdims=True) + EPSILON)
    return (wide * inverse * gain_rows).astype(jnp.bfloat16)


def fused_kernel(
    devices, segment_hbm, query_hbm, key_hbm, value_hbm,
    text_hbm, hidden_hbm, query_gain_hbm, key_gain_hbm, gate_hbm, out_ref,
    text_ref, hidden_ref, query_gain_ref, key_gain_ref, gate_ref,
    staged, shared, owned, weights, shared_out, owned_out, back, seg_all, hot, earlier,
    query_gains, key_gains, bias, gate_rows,
    level_sem, row_sem, across_sem, core_sem, pair_sem,
    load_sem, seg_own_sem, stage_sem, slot_sem,
    seg_send, seg_recv, send_sem, recv_sem, relay_send, relay_recv,
):
    chips = devices // 2
    levels = chips // 2
    tok = hidden_hbm.shape[0]
    per_chip = hidden_hbm.shape[1] // HEAD_DIM // chips
    own_heads = per_chip // 2
    requests = gate_hbm.shape[0]
    tokens = devices * tok
    me = lax.axis_index("seq")
    chip, core = me // 2, me % 2
    row, level = chip % 2, chip // 2
    partner = me + 1 - 2 * core
    sources = (query_hbm, key_hbm, value_hbm)

    def columns(head):
        return pl.ds(pl.multiple_of(head * HEAD_DIM, HEAD_DIM), HEAD_DIM)

    def chip_at(a_level, a_row):
        return a_level * 2 + a_row

    def signal(semaphore, device):
        pl.semaphore_signal(
            semaphore, inc=1, device_id={"seq": device}, device_id_type=pl.DeviceIdType.MESH
        )

    def remote(src, dst, send, recv, device):
        copy = pltpu.make_async_remote_copy(
            src_ref=src, dst_ref=dst, send_sem=send, recv_sem=recv,
            device_id={"seq": device}, device_id_type=pl.DeviceIdType.MESH,
        )
        copy.start()
        return copy

    def settle(ref, semaphore):
        pltpu.make_async_copy(ref, ref, semaphore).wait()

    toward = 1 - 2 * (level // (levels // 2))
    near_first = [(level + levels + toward * step) % levels for step in range(1, levels)]
    far_first = [(level + levels - toward * step) % levels for step in range(1, levels)]

    barrier = pltpu.get_barrier_semaphore()
    for step in range(1, levels):
        @pl.when(level + step < levels)
        def _():
            signal(barrier, chip_at(level + step, row) * 2 + core)

    @pl.when(row == 0)
    def _():
        signal(barrier, chip_at(level, 1) * 2 + core)

    @pl.when(core == 0)
    def _():
        signal(barrier, partner)

    seg_own = pltpu.make_async_copy(segment_hbm, seg_all.at[chip, core], seg_own_sem)
    seg_own.start()
    for part, source in enumerate(sources):
        pltpu.make_async_copy(source, staged.at[part], stage_sem.at[part // 2]).start()
    for part, source in enumerate(sources):
        pltpu.make_async_copy(
            source.at[:, columns(chip * per_chip)], shared.at[part, chip, core], slot_sem.at[0]
        ).start()
        for j in range(own_heads):
            pltpu.make_async_copy(
                source.at[:, columns(chip * per_chip + 1 + core * own_heads + j)],
                owned.at[j, part, chip, core], slot_sem.at[1 + j],
            ).start()
    loads = [
        pltpu.make_async_copy(source, target, load_sem.at[place])
        for place, (source, target) in enumerate(
            (
                (text_hbm, text_ref), (query_gain_hbm, query_gain_ref),
                (key_gain_hbm, key_gain_ref), (gate_hbm, gate_ref), (hidden_hbm, hidden_ref),
            )
        )
    ]
    for copy in loads:
        copy.start()
    seg_own.wait()
    settle(staged.at[0:2], stage_sem.at[0])

    @pl.when(me > 0)
    def _():
        pl.semaphore_wait(barrier, level + row + core)

    for step in range(1, levels):
        @pl.when(level >= step)
        def _():
            signal(level_sem.at[level], chip_at(level - step, row) * 2 + core)

    @pl.when(row == 1)
    def _():
        signal(row_sem, chip_at(level, 0) * 2 + core)

    @pl.when(core == 1)
    def _():
        signal(core_sem, partner)

    seg_copies = []

    def send_shared(to_chip):
        seg_copies.append(remote(
            seg_all.at[chip, core], seg_all.at[chip, core],
            seg_send.at[len(seg_copies)], seg_recv.at[chip], to_chip * 2 + core,
        ))
        remote(
            staged.at[0:2, :, columns(to_chip * per_chip)], shared.at[0:2, chip, core],
            send_sem.at[0], recv_sem.at[0], to_chip * 2 + core,
        )

    def meet(a_level):
        @pl.when(a_level > level)
        def _():
            pl.semaphore_wait(level_sem.at[a_level], 1)

    meet(near_first[0])
    send_shared(chip_at(near_first[0], row))

    @pl.when(row == 0)
    def _():
        pl.semaphore_wait(row_sem, 1)

    signal(across_sem.at[level], chip_at(near_first[0], row) * 2 + core)
    send_shared(chip_at(level, 1 - row))
    for a_level in near_first[1:]:
        meet(a_level)
        signal(across_sem.at[level], chip_at(a_level, row) * 2 + core)
        send_shared(chip_at(a_level, row))
    for a_level in near_first:
        pl.semaphore_wait(across_sem.at[a_level], 1)
        send_shared(chip_at(a_level, 1 - row))

    near_chips = [chip_at(a, row) for a in near_first] + [chip_at(level, 1 - row)]
    near_chips += [chip_at(a, 1 - row) for a in near_first]
    far_chips = [chip_at(a, 1 - row) for a in far_first] + [chip_at(a, row) for a in far_first]
    far_chips += [chip_at(level, 1 - row)]

    settle(staged.at[2], stage_sem.at[1])
    for to_chip in near_chips:
        remote(
            staged.at[2, :, columns(to_chip * per_chip)], shared.at[2, chip, core],
            send_sem.at[1], recv_sem.at[1], to_chip * 2 + core,
        )

    @pl.when(core == 0)
    def _():
        pl.semaphore_wait(core_sem, 1)

    for to_chip in near_chips:
        signal(pair_sem, to_chip * 2 + core)

    def own_head(j, a_core):
        return 1 + a_core * own_heads + j

    beside = [
        remote(
            staged.at[:, :, columns(chip * per_chip + own_head(j, 1 - core))],
            owned.at[j, :, chip, core], relay_send.at[3 + j], relay_recv.at[3 + j], partner,
        )
        for j in range(own_heads)
    ]

    earlier[...] = (
        lax.broadcasted_iota(jnp.int32, (tokens, tokens), 1)
        < lax.broadcasted_iota(jnp.int32, (tokens, tokens), 0)
    ).astype(jnp.float32).astype(jnp.bfloat16)

    pl.semaphore_wait(pair_sem, chips - 1)
    for j in range(own_heads):
        for to_chip in near_chips:
            for a_core in range(2):
                remote(
                    staged.at[0:2, :, columns(to_chip * per_chip + own_head(j, a_core))],
                    owned.at[j, 0:2, chip, core],
                    send_sem.at[4 + 2 * j], recv_sem.at[4 + 2 * j], to_chip * 2 + a_core,
                )
    for j in range(own_heads):
        for to_chip in far_chips:
            for a_core in range(2):
                remote(
                    staged.at[2, :, columns(to_chip * per_chip + own_head(j, a_core))],
                    owned.at[j, 2, chip, core],
                    send_sem.at[5 + 2 * j], recv_sem.at[5 + 2 * j], to_chip * 2 + a_core,
                )

    for step in range(1, chips):
        source = (chip + step) % chips
        settle(seg_all.at[source, core], seg_recv.at[source])
    seg_relay = remote(
        seg_all.at[:, core], seg_all.at[:, core], relay_send.at[0], relay_recv.at[0], partner
    )
    for copy in loads:
        copy.wait()
    seg_relay.wait_recv()
    eye = (
        lax.broadcasted_iota(jnp.int32, (tok, tok), 0)
        == lax.broadcasted_iota(jnp.int32, (tok, tok), 1)
    ).astype(jnp.float32).astype(jnp.bfloat16)
    ids = lax.broadcasted_iota(jnp.int32, (LANES, tok), 0)
    for n in range(devices):
        flipped = (ids == seg_all[n // 2, n % 2]).astype(jnp.float32).astype(jnp.bfloat16)
        hot[n] = lax.dot_general(
            eye, flipped, CONTRACT_LAST, preferred_element_type=jnp.float32
        ).astype(jnp.bfloat16)
    all_hot = hot[...].reshape(tokens, LANES)
    before = jnp.dot(earlier[...], all_hot, preferred_element_type=jnp.float32)
    lane = lax.broadcasted_iota(jnp.int32, (1, LANES), 1)
    limit = jnp.zeros((1, LANES), jnp.int32)
    for r in range(requests):
        limit = jnp.where(lane == r, text_ref[0:1, r : r + 1], limit)
    inside = jnp.where(before < limit.astype(jnp.float32), all_hot.astype(jnp.float32), 0.0)
    text = jnp.dot(
        inside.astype(jnp.bfloat16), jnp.ones((LANES, LANES), jnp.bfloat16),
        preferred_element_type=jnp.float32,
    ) > 0.5
    query_gain, key_gain = query_gain_ref[...], key_gain_ref[...]
    spread = (chips, 2, tok, LANES)
    query_gains[...] = jnp.where(text, query_gain[0:1], query_gain[1:2]).reshape(spread)
    key_gains[...] = jnp.where(text, key_gain[0:1], key_gain[1:2]).reshape(spread)
    same = lax.dot_general(all_hot, all_hot, CONTRACT_LAST, preferred_element_type=jnp.float32)
    bias[...] = jnp.where(same > 0.5, 0.0, MASKED).reshape(chips, 2, tok, tokens)

    scale = 1.0 / math.sqrt(HEAD_DIM)

    def attention_weights(query_n, key_n, query_bias):
        scores = lax.dot_general(
            query_n, key_n, CONTRACT_LAST, preferred_element_type=jnp.float32
        ) * scale + query_bias
        grown = jnp.exp(scores - jnp.max(scores, axis=-1, keepdims=True))
        return (grown * (1.0 / jnp.sum(grown, axis=-1, keepdims=True))).astype(jnp.bfloat16)

    settle(shared.at[:, chip, core], slot_sem.at[0])
    settle(shared.at[0:2, 0 : chips - 1, 0], recv_sem.at[0])
    relays = [remote(
        shared.at[1, :, core], shared.at[1, :, core], relay_send.at[1], relay_recv.at[1], partner
    )]
    settle(shared.at[2, 0 : chips - 1, 0], recv_sem.at[1])
    relays.append(remote(
        shared.at[2, :, core], shared.at[2, :, core], relay_send.at[2], relay_recv.at[2], partner
    ))
    half = (tokens // 2, HEAD_DIM)
    full = (tokens, HEAD_DIM)
    query_n = normed(shared.at[0, :, core][...], query_gains.at[:, core][...]).reshape(half)
    relays[0].wait_recv()
    key_n = normed(shared[1], key_gains[...]).reshape(full)
    part_weights = attention_weights(
        query_n, key_n, bias.at[:, core][...].reshape(tokens // 2, tokens)
    )
    relays[1].wait_recv()
    shared_out[...] = jnp.dot(
        part_weights, shared[2].reshape(full), preferred_element_type=jnp.float32
    ).astype(jnp.bfloat16).reshape(chips, tok, HEAD_DIM)
    for to_chip in far_chips:
        remote(
            shared_out.at[to_chip], back.at[chip * per_chip],
            send_sem.at[2], recv_sem.at[2], to_chip * 2 + core,
        )

    number = lax.broadcasted_iota(jnp.int32, (LANES, LANES), 0).astype(jnp.float32)
    own_id = jnp.dot(hot[me], number.astype(jnp.bfloat16), preferred_element_type=jnp.float32)
    own_before = jnp.dot(
        earlier[pl.ds(pl.multiple_of(me * tok, tok), tok), :], all_hot,
        preferred_element_type=jnp.float32,
    )
    own_inside = jnp.where(
        own_before < limit.astype(jnp.float32), hot[me].astype(jnp.float32), 0.0
    )
    own_text = jnp.dot(
        own_inside.astype(jnp.bfloat16), jnp.ones((LANES, LANES), jnp.bfloat16),
        preferred_element_type=jnp.float32,
    )
    own_code = 2.0 * own_id + jnp.where(own_text > 0.5, 0.0, 1.0)
    for tile in range(hidden_ref.shape[1] // LANES):
        cols = slice(tile * LANES, (tile + 1) * LANES)
        total = jnp.zeros((tok, LANES), jnp.float32)
        for r in range(requests):
            pair = gate_ref[r, :, cols].astype(jnp.float32)
            for s in range(2):
                total = jnp.where(own_code == float(2 * r + s), pair[s : s + 1], total)
        gate_rows[tile] = total

    for j in range(own_heads):
        settle(owned.at[j, :, chip, core], slot_sem.at[1 + j])
        settle(owned.at[j, 0:2, 0 : chips - 1], recv_sem.at[4 + 2 * j])
        beside[j].wait_recv()
        query_n = normed(owned[j, 0], query_gains[...]).reshape(full)
        key_n = normed(owned[j, 1], key_gains[...]).reshape(full)
        weights[j] = attention_weights(query_n, key_n, bias[...].reshape(tokens, tokens))
    for j in range(own_heads):
        settle(owned.at[j, 2, 0 : chips - 1], recv_sem.at[5 + 2 * j])
        owned_out[j] = jnp.dot(
            weights[j], owned[j, 2].reshape(full), preferred_element_type=jnp.float32
        ).astype(jnp.bfloat16).reshape(chips, 2, tok, HEAD_DIM)
        head = chip * per_chip + own_head(j, core)
        for to_chip in far_chips:
            for a_core in range(2):
                remote(
                    owned_out.at[j, to_chip, a_core], back.at[head],
                    send_sem.at[3], recv_sem.at[3], to_chip * 2 + a_core,
                )
        remote(
            owned_out.at[j, chip, 1 - core], back.at[head],
            send_sem.at[3], recv_sem.at[3], partner,
        )

    def finish(head):
        cols = slice(head * HEAD_DIM, (head + 1) * HEAD_DIM)
        out_ref[:, cols] = (
            hidden_ref[:, cols].astype(jnp.float32)
            + gate_rows[head] * back[head].astype(jnp.float32)
        ).astype(jnp.bfloat16)

    back[chip * per_chip] = shared_out[chip]
    settle(back.at[0 : chips - 1], recv_sem.at[2])
    for a_chip in range(chips):
        finish(a_chip * per_chip)
    for j in range(own_heads):
        back[chip * per_chip + own_head(j, core)] = owned_out.at[j, chip, core][...]
    settle(back.at[0 : own_heads * (devices - 1)], recv_sem.at[3])
    for a_chip in range(chips):
        for head in range(1, per_chip):
            finish(a_chip * per_chip + head)

    for copy in seg_copies + [seg_relay] + relays + beside:
        copy.wait_send()
    settle(shared.at[0:2, 0 : chips - 1, 0], send_sem.at[0])
    settle(shared.at[2, 0 : chips - 1, 0], send_sem.at[1])
    settle(back.at[0 : chips - 1], send_sem.at[2])
    settle(back.at[0 : own_heads * (devices - 1)], send_sem.at[3])
    for j in range(own_heads):
        settle(owned.at[j, 0:2, 0 : chips - 1], send_sem.at[4 + 2 * j])
        settle(owned.at[j, 2, 0 : chips - 1], send_sem.at[5 + 2 * j])


def fused(
    hidden, queries, key_rows, values, query_gain, key_gain, gate_table, segment, text_count
):
    devices = lax.axis_size("seq")
    chips = devices // 2
    levels = chips // 2
    tok, width = hidden.shape
    heads = width // HEAD_DIM
    own_heads = heads // chips // 2
    tokens = devices * tok
    hbm = pl.BlockSpec(memory_space=pl.ANY)
    block = (tok, HEAD_DIM)
    dma = pltpu.SemaphoreType.DMA
    regular = pltpu.SemaphoreType.REGULAR
    return pl.pallas_call(
        functools.partial(fused_kernel, devices),
        out_shape=jax.ShapeDtypeStruct((tok, width), jnp.bfloat16),
        in_specs=[hbm] * 9,
        out_specs=pl.BlockSpec(memory_space=pltpu.VMEM),
        scratch_shapes=[
            pltpu.VMEM((1, text_count.shape[0]), jnp.int32),
            pltpu.VMEM(hidden.shape, hidden.dtype),
            pltpu.VMEM(query_gain.shape, query_gain.dtype),
            pltpu.VMEM(key_gain.shape, key_gain.dtype),
            pltpu.VMEM(gate_table.shape, gate_table.dtype),
            pltpu.VMEM((3, tok, width), jnp.bfloat16),
            pltpu.VMEM((3, chips, 2) + block, jnp.bfloat16),
            pltpu.VMEM((own_heads, 3, chips, 2) + block, jnp.bfloat16),
            pltpu.VMEM((own_heads, tokens, tokens), jnp.bfloat16),
            pltpu.VMEM((chips,) + block, jnp.bfloat16),
            pltpu.VMEM((own_heads, chips, 2) + block, jnp.bfloat16),
            pltpu.VMEM((heads,) + block, jnp.bfloat16),
            pltpu.VMEM((chips, 2, 1, tok), jnp.int32),
            pltpu.VMEM((devices, tok, LANES), jnp.bfloat16),
            pltpu.VMEM((tokens, tokens), jnp.bfloat16),
            pltpu.VMEM((chips, 2, tok, LANES), jnp.float32),
            pltpu.VMEM((chips, 2, tok, LANES), jnp.float32),
            pltpu.VMEM((chips, 2, tok, tokens), jnp.float32),
            pltpu.VMEM((heads, tok, LANES), jnp.float32),
            regular((levels,)),
            regular,
            regular((levels,)),
            regular,
            regular,
            dma((5,)),
            dma,
            dma((2,)),
            dma((1 + own_heads,)),
            dma((chips - 1,)),
            dma((chips,)),
            dma((4 + 2 * own_heads,)),
            dma((4 + 2 * own_heads,)),
            dma((3 + own_heads,)),
            dma((3 + own_heads,)),
        ],
        compiler_params=pltpu.CompilerParams(
            collective_id=0, has_side_effects=True, vmem_limit_bytes=16 * 1024 * 1024
        ),
    )(*(
        pltpu.with_memory_space_constraint(array, pltpu.HBM)
        for array in (
            segment.reshape(1, tok), queries, key_rows, values,
            text_count.reshape(1, -1), hidden, query_gain, key_gain, gate_table,
        )
    ))


def program(*arrays):
    devices = lax.axis_size("seq")
    tok, width = arrays[0].shape
    requests = arrays[-1].shape[0]
    whole_heads = devices % 8 == 0 and (width // HEAD_DIM) % (devices // 2) == 0
    odd = whole_heads and width // HEAD_DIM // (devices // 2) % 2 == 1
    if odd and devices * tok <= 512 and requests <= LANES and tok % 16 == 0:
        return fused(*arrays)
    return per_device(*arrays)


def solution(mesh):
    return jax.shard_map(
        program,
        mesh=mesh,
        in_specs=(
            P(("groups", "seq"), None),
            P(("groups", "seq"), None),
            P(("groups", "seq"), None),
            P(("groups", "seq"), None),
            P(),
            P(),
            P("groups", None, None),
            P(("groups", "seq")),
            P("groups"),
        ),
        out_specs=P(("groups", "seq"), None),
        check_vma=False,
    )
```

```python
import functools
import math

import jax
import jax.numpy as jnp
from jax import lax
from jax.experimental import pallas as pl
from jax.experimental.pallas import tpu as pltpu
from jax.sharding import PartitionSpec as P

HEAD_DIM = 128


EPSILON = 1e-06
MASKED = -1e30


def head_norm(rows_in, gains, stream):
    row_count = rows_in.shape[0]
    per_head = rows_in.astype(jnp.float32).reshape(row_count, -1, HEAD_DIM)
    inverse = lax.rsqrt(jnp.mean(per_head * per_head, axis=-1, keepdims=True) + EPSILON)
    gain_rows = jnp.where((stream == 0)[:, None], gains[0][None, :], gains[1][None, :])
    return (per_head * inverse * gain_rows[:, None, :]).astype(jnp.bfloat16).reshape(row_count, -1)


def attend(query_block, block_segment, key_data, value_data, key_segment):
    scores = jnp.einsum(
        "qhd,khd->hqk", query_block, key_data, preferred_element_type=jnp.float32
    ) * (1.0 / math.sqrt(HEAD_DIM))
    allowed = (block_segment[:, None] == key_segment[None, :])[None, :, :]
    scores = jnp.where(allowed, scores, MASKED)
    largest = jnp.max(scores, axis=-1, keepdims=True)
    weights = jnp.exp(scores - largest)
    weights = (weights / jnp.sum(weights, axis=-1, keepdims=True)).astype(jnp.bfloat16)
    return jnp.einsum(
        "hqk,khd->qhd", weights, value_data, preferred_element_type=jnp.float32
    ).astype(jnp.bfloat16)


def per_device(
    hidden, queries, key_rows, values, query_gain, key_gain, gate_table, segment, text_count
):
    tok_rows = hidden.shape[0]
    width_all = hidden.shape[1]
    devices = lax.axis_size("seq")
    requests = text_count.shape[0]
    seg_hot = (segment[:, None] == jnp.arange(requests, dtype=jnp.int32)[None, :]).astype(jnp.int32)
    local_counts = jnp.sum(seg_hot, axis=0)
    all_counts = lax.all_gather(local_counts[None, :], "seq", axis=0, tiled=True)
    lower_rows = (jnp.arange(devices, dtype=jnp.int32) < lax.axis_index("seq")).astype(jnp.int32)
    before = jnp.sum(all_counts * lower_rows[:, None], axis=0)
    position = jnp.sum((jnp.cumsum(seg_hot, axis=0) - seg_hot + before[None, :]) * seg_hot, axis=1)
    text_limit = jnp.sum(seg_hot * text_count[None, :], axis=1)
    stream = (position >= text_limit).astype(jnp.int32)
    query_normed = head_norm(queries, query_gain, stream)
    key_normed = head_norm(key_rows, key_gain, stream)
    groups = 8
    pair_merge = 2
    slices = devices // groups
    cap_rows = 4 * tok_rows // devices + max(1, tok_rows // devices)
    bucket_rows = cap_rows * pair_merge
    head_cols = width_all // groups
    owner_slice = segment // pair_merge
    owner_hot = (owner_slice[:, None] == jnp.arange(slices, dtype=jnp.int32)[None, :]).astype(
        jnp.int32
    )
    owner_rank = jnp.sum((jnp.cumsum(owner_hot, axis=0) - owner_hot) * owner_hot, axis=1)
    slot_place = owner_slice * bucket_rows + owner_rank
    bucket_index = (
        jnp.full((slices * bucket_rows,), tok_rows, jnp.int32)
        .at[slot_place]
        .set(jnp.arange(tok_rows, dtype=jnp.int32))
    )
    stacked = jnp.concatenate(
        [
            query_normed.reshape(tok_rows, groups, head_cols),
            key_normed.reshape(tok_rows, groups, head_cols),
            values.reshape(tok_rows, groups, head_cols),
        ],
        axis=2,
    ).transpose(1, 0, 2)
    outgoing = jnp.take(stacked, bucket_index, axis=1, mode="fill", fill_value=0).reshape(
        devices, bucket_rows, 3 * head_cols
    )
    slot_segment = jnp.take(segment, bucket_index, axis=0, mode="fill", fill_value=-1)
    segment_out = jnp.broadcast_to(slot_segment[None, :], (groups, slices * bucket_rows)).reshape(
        devices, bucket_rows
    )
    arrived, arrived_segment = (
        lax.all_to_all(outgoing, "seq", split_axis=0, concat_axis=0, tiled=True),
        lax.all_to_all(segment_out, "seq", split_axis=0, concat_axis=0, tiled=True),
    )
    slot_count = devices * bucket_rows
    per_head = head_cols // HEAD_DIM
    slot_data = arrived.reshape(slot_count, 3 * head_cols)
    query_all = slot_data[:, :head_cols].reshape(slot_count, per_head, HEAD_DIM)
    key_all = slot_data[:, head_cols : 2 * head_cols].reshape(slot_count, per_head, HEAD_DIM)
    value_all = slot_data[:, 2 * head_cols :].reshape(slot_count, per_head, HEAD_DIM)
    key_segment = arrived_segment.reshape(slot_count)
    if slot_count % 512 == 0:
        block_rows = 512
    elif slot_count % 256 == 0:
        block_rows = 256
    else:
        block_rows = slot_count

    def one_block(first_row):
        return attend(query_all, key_segment, key_all, value_all, key_segment)

    results = lax.map(one_block, jnp.arange(slot_count // block_rows, dtype=jnp.int32) * block_rows)
    returning = results.reshape(devices, bucket_rows, head_cols)
    returned = lax.all_to_all(returning, "seq", split_axis=0, concat_axis=0, tiled=True)
    returned = returned.reshape(groups, slices * bucket_rows, head_cols)
    attention = (
        jnp.take(returned, slot_place, axis=1).transpose(1, 0, 2).reshape(tok_rows, width_all)
    )
    gate_rows = jnp.take(gate_table.reshape(requests * 2, width_all), segment * 2 + stream, axis=0)
    mixed = hidden.astype(jnp.float32) + gate_rows.astype(jnp.float32) * attention.astype(
        jnp.float32
    )
    return mixed.astype(jnp.bfloat16)


LANES = 128
CONTRACT_LAST = (((1,), (1,)), ((), ()))
FIRST_CORE = (1, 0)


def normed(rows, gain_rows):
    wide = rows.astype(jnp.float32)
    inverse = lax.rsqrt(jnp.mean(wide * wide, axis=-1, keepdims=True) + EPSILON)
    return (wide * inverse * gain_rows).astype(jnp.bfloat16)


def fused_kernel(
    devices, segment_hbm, query_hbm, key_hbm, value_hbm,
    text_hbm, hidden_hbm, query_gain_hbm, key_gain_hbm, gate_hbm, out_ref,
    text_ref, hidden_ref, query_gain_ref, key_gain_ref, gate_ref,
    staged, shared, owned, weights, shared_out, owned_out, back, seg_all, hot, earlier,
    query_gains, key_gains, bias, gate_rows,
    here_sem, go_sem, load_sem, seg_own_sem, stage_sem, slot_sem,
    seg_send, seg_recv, send_sem, recv_sem, relay_send, relay_recv,
):
    chips = devices // 2
    levels = chips // 2
    tok = hidden_hbm.shape[0]
    per_chip = hidden_hbm.shape[1] // HEAD_DIM // chips
    own_heads = per_chip // 2
    requests = gate_hbm.shape[0]
    tokens = devices * tok
    me = lax.axis_index("seq")
    chip, core = me // 2, me % 2
    row, level = chip % 2, chip // 2
    partner = me + 1 - 2 * core
    sources = (query_hbm, key_hbm, value_hbm)

    def columns(head):
        return pl.ds(pl.multiple_of(head * HEAD_DIM, HEAD_DIM), HEAD_DIM)

    def chip_at(a_level, a_row):
        return a_level * 2 + a_row

    def signal(semaphore, device):
        pl.semaphore_signal(
            semaphore, inc=1, device_id={"seq": device}, device_id_type=pl.DeviceIdType.MESH
        )

    def remote(src, dst, send, recv, device):
        copy = pltpu.make_async_remote_copy(
            src_ref=src, dst_ref=dst, send_sem=send, recv_sem=recv,
            device_id={"seq": device}, device_id_type=pl.DeviceIdType.MESH,
        )
        copy.start()
        return copy

    def settle(ref, semaphore):
        pltpu.make_async_copy(ref, ref, semaphore).wait()

    toward = 1 - 2 * (level // (levels // 2))
    near_first = [(level + levels + toward * step) % levels for step in range(1, levels)]
    far_first = [(level + levels - toward * step) % levels for step in range(1, levels)]
    orders = []
    for start in range(levels):
        first = start + (1 if start < levels // 2 else -1)
        rest = list(range(start - 1, -1, -1)) + list(range(start + 1, levels))
        orders.append([first] + [n for n in rest if n != first])

    def pick(values):
        result = values[0]
        for start in range(1, levels):
            result = jnp.where(level == start, values[start], result)
        return result

    met = [pick([order[place] for order in orders]) for place in range(levels - 1)]
    near_chips = []
    for place, a_level in enumerate(near_first):
        near_chips.append(chip_at(a_level, row))
        near_chips.append(chip_at(a_level, 1 - row))
    near_chips.append(chip_at(level, 1 - row))
    far_chips = []
    for a_level in far_first:
        far_chips += [chip_at(a_level, 1 - row), chip_at(a_level, row)]
    far_chips.append(chip_at(level, 1 - row))

    for part in range(2):
        pltpu.make_async_copy(sources[part], staged.at[part], stage_sem.at[0]).start()

    barrier = pltpu.get_barrier_semaphore()

    @pl.when(me > 0)
    def _():
        pl.semaphore_wait(barrier, (level + levels - 1) // levels + row + core)

    @pl.when(level + 1 < levels)
    def _():
        signal(barrier, me + 4)

    @pl.when(row == 0)
    def _():
        signal(barrier, me + 2)

    @pl.when(core == 0)
    def _():
        signal(barrier, me + 1)

    for down in range(levels):
        for row_down in range(2):
            for core_down in range(2):
                if down + row_down + core_down > 0:
                    fits = level >= down
                    if row_down:
                        fits = jnp.logical_and(fits, row == 1)
                    if core_down:
                        fits = jnp.logical_and(fits, core == 1)

                    @pl.when(fits)
                    def _():
                        signal(here_sem.at[me], me - 4 * down - 2 * row_down - core_down)

    def vouched(condition, a_level, a_row, a_core):
        @pl.when(condition)
        def _():
            pl.semaphore_wait(here_sem.at[chip_at(a_level, a_row) * 2 + a_core], 1)

    seg_own = pltpu.make_async_copy(segment_hbm, seg_all.at[chip, core], seg_own_sem)
    seg_own.start()
    pltpu.make_async_copy(sources[2], staged.at[2], stage_sem.at[1]).start()
    for part, source in enumerate(sources):
        pltpu.make_async_copy(
            source.at[:, columns(chip * per_chip)], shared.at[part, chip, core], slot_sem.at[0]
        ).start()
        for j in range(own_heads):
            pltpu.make_async_copy(
                source.at[:, columns(chip * per_chip + 1 + core * own_heads + j)],
                owned.at[j, part, chip, core], slot_sem.at[1 + j],
            ).start()
    loads = [
        pltpu.make_async_copy(source, target, load_sem.at[place])
        for place, (source, target) in enumerate(
            (
                (text_hbm, text_ref), (query_gain_hbm, query_gain_ref),
                (key_gain_hbm, key_gain_ref), (gate_hbm, gate_ref), (hidden_hbm, hidden_ref),
            )
        )
    ]
    for copy in loads:
        copy.start()
    settle(staged.at[0:2], stage_sem.at[0])
    seg_own.wait()

    seg_copies = []

    def own_head(j, a_core):
        return 1 + a_core * own_heads + j

    def send_owned(parts, place, j, to_chip, a_core):
        remote(
            staged.at[parts, :, columns(to_chip * per_chip + own_head(j, a_core))],
            owned.at[j, parts, chip, core],
            send_sem.at[place + 2 * j], recv_sem.at[place + 2 * j], to_chip * 2 + a_core,
        )

    def send_shared(to_chip):
        seg_copies.append(remote(
            seg_all.at[chip, core], seg_all.at[chip, core],
            seg_send.at[len(seg_copies)], seg_recv.at[chip], to_chip * 2 + core,
        ))
        cols = columns(to_chip * per_chip)
        remote(
            staged.at[0:2, :, cols], shared.at[0:2, chip, core],
            send_sem.at[0], recv_sem.at[0], to_chip * 2 + core,
        )
        remote(
            staged.at[2, :, cols], shared.at[2, chip, core],
            send_sem.at[1], recv_sem.at[1], to_chip * 2 + core,
        )

    settle(staged.at[2], stage_sem.at[1])
    low = core == 0
    upper = row == 0
    low_upper = jnp.logical_and(low, upper)

    def send_query_key(to_chip, a_core):
        for j in range(own_heads):
            send_owned(slice(0, 2), 5, j, to_chip, a_core)

    def send_value(to_chip, a_core):
        for j in range(own_heads):
            send_owned(2, 6, j, to_chip, a_core)

    def send_all_owned(to_chips):
        for to_chip in to_chips:
            send_query_key(to_chip, FIRST_CORE[0])
            send_value(to_chip, FIRST_CORE[0])
        for to_chip in to_chips:
            send_query_key(to_chip, FIRST_CORE[1])
        for to_chip in to_chips:
            send_value(to_chip, FIRST_CORE[1])

    beside = []
    for place, a_level in enumerate(met):
        above = a_level > level
        vouched(above, a_level, row, core)
        send_shared(chip_at(a_level, row))
        if place == 0:
            vouched(low, level, row, 1)
            vouched(jnp.logical_and(low, above), a_level, row, 1)
            send_all_owned([chip_at(a_level, row)])
            continue
        if place == 1:
            vouched(upper, level, 1, core)
            send_shared(chip_at(level, 1 - row))
            vouched(jnp.logical_and(met[0] > level, upper), met[0], 1, core)
            send_shared(chip_at(met[0], 1 - row))
        vouched(jnp.logical_and(above, upper), a_level, 1, core)
        send_shared(chip_at(a_level, 1 - row))

    for j in range(own_heads):
        beside.append(remote(
            staged.at[:, :, columns(chip * per_chip + own_head(j, 1 - core))],
            owned.at[j, :, chip, core], relay_send.at[3 + j], relay_recv.at[3 + j], partner,
        ))
    vouched(low_upper, level, 1, 1)
    vouched(jnp.logical_and(low_upper, met[0] > level), met[0], 1, 1)
    for a_level in met[1:]:
        vouched(jnp.logical_and(low, a_level > level), a_level, row, 1)
        vouched(jnp.logical_and(low_upper, a_level > level), a_level, 1, 1)

    across_chips = []
    for a_level in met[1:]:
        across_chips += [chip_at(a_level, row), chip_at(a_level, 1 - row)]
    beside_chips = [chip_at(met[0], 1 - row), chip_at(level, 1 - row)]
    inner = jnp.logical_or(level == levels // 2 - 1, level == levels // 2)

    @pl.when(inner)
    def _():
        send_all_owned(beside_chips[0:1] + across_chips + beside_chips[1:])

    @pl.when(jnp.logical_not(inner))
    def _():
        send_all_owned(beside_chips)

    earlier[...] = (
        lax.broadcasted_iota(jnp.int32, (tokens, tokens), 1)
        < lax.broadcasted_iota(jnp.int32, (tokens, tokens), 0)
    ).astype(jnp.float32).astype(jnp.bfloat16)

    shared_sends = (shared.at[0:2, 0 : chips - 1, 0], shared.at[2, 0 : chips - 1, 0])

    @pl.when(inner)
    def _():
        for place in range(2):
            settle(shared_sends[place], send_sem.at[place])
        for step in range(1, levels // 2):
            signal(go_sem, chip_at(level - toward * step, row) * 2 + core)

    @pl.when(jnp.logical_not(inner))
    def _():
        pl.semaphore_wait(go_sem, 1)
        send_all_owned(across_chips)

    for step in range(1, chips):
        source = (chip + step) % chips
        settle(seg_all.at[source, core], seg_recv.at[source])
    seg_relay = remote(
        seg_all.at[:, core], seg_all.at[:, core], relay_send.at[0], relay_recv.at[0], partner
    )
    for copy in loads:
        copy.wait()
    seg_relay.wait_recv()
    eye = (
        lax.broadcasted_iota(jnp.int32, (tok, tok), 0)
        == lax.broadcasted_iota(jnp.int32, (tok, tok), 1)
    ).astype(jnp.float32).astype(jnp.bfloat16)
    ids = lax.broadcasted_iota(jnp.int32, (LANES, tok), 0)
    for n in range(devices):
        flipped = (ids == seg_all[n // 2, n % 2]).astype(jnp.float32).astype(jnp.bfloat16)
        hot[n] = lax.dot_general(
            eye, flipped, CONTRACT_LAST, preferred_element_type=jnp.float32
        ).astype(jnp.bfloat16)
    all_hot = hot[...].reshape(tokens, LANES)
    before = jnp.dot(earlier[...], all_hot, preferred_element_type=jnp.float32)
    lane = lax.broadcasted_iota(jnp.int32, (1, LANES), 1)
    limit = jnp.zeros((1, LANES), jnp.int32)
    for r in range(requests):
        limit = jnp.where(lane == r, text_ref[0:1, r : r + 1], limit)
    inside = jnp.where(before < limit.astype(jnp.float32), all_hot.astype(jnp.float32), 0.0)
    text = jnp.dot(
        inside.astype(jnp.bfloat16), jnp.ones((LANES, LANES), jnp.bfloat16),
        preferred_element_type=jnp.float32,
    ) > 0.5
    query_gain, key_gain = query_gain_ref[...], key_gain_ref[...]
    spread = (chips, 2, tok, LANES)
    query_gains[...] = jnp.where(text, query_gain[0:1], query_gain[1:2]).reshape(spread)
    key_gains[...] = jnp.where(text, key_gain[0:1], key_gain[1:2]).reshape(spread)
    same = lax.dot_general(all_hot, all_hot, CONTRACT_LAST, preferred_element_type=jnp.float32)
    bias[...] = jnp.where(same > 0.5, 0.0, MASKED).reshape(chips, 2, tok, tokens)

    scale = 1.0 / math.sqrt(HEAD_DIM)

    def attention_weights(query_n, key_n, query_bias):
        scores = lax.dot_general(
            query_n, key_n, CONTRACT_LAST, preferred_element_type=jnp.float32
        ) * scale + query_bias
        grown = jnp.exp(scores - jnp.max(scores, axis=-1, keepdims=True))
        return (grown * (1.0 / jnp.sum(grown, axis=-1, keepdims=True))).astype(jnp.bfloat16)

    settle(shared.at[:, chip, core], slot_sem.at[0])
    settle(shared.at[0:2, 0 : chips - 1, 0], recv_sem.at[0])
    relays = [remote(
        shared.at[1, :, core], shared.at[1, :, core], relay_send.at[1], relay_recv.at[1], partner
    )]
    settle(shared.at[2, 0 : chips - 1, 0], recv_sem.at[1])
    relays.append(remote(
        shared.at[2, :, core], shared.at[2, :, core], relay_send.at[2], relay_recv.at[2], partner
    ))
    half = (tokens // 2, HEAD_DIM)
    full = (tokens, HEAD_DIM)
    query_n = normed(shared.at[0, :, core][...], query_gains.at[:, core][...]).reshape(half)
    relays[0].wait_recv()
    key_n = normed(shared[1], key_gains[...]).reshape(full)
    part_weights = attention_weights(
        query_n, key_n, bias.at[:, core][...].reshape(tokens // 2, tokens)
    )
    relays[1].wait_recv()
    shared_out[...] = jnp.dot(
        part_weights, shared[2].reshape(full), preferred_element_type=jnp.float32
    ).astype(jnp.bfloat16).reshape(chips, tok, HEAD_DIM)

    number = lax.broadcasted_iota(jnp.int32, (LANES, LANES), 0).astype(jnp.float32)
    own_id = jnp.dot(hot[me], number.astype(jnp.bfloat16), preferred_element_type=jnp.float32)
    own_before = jnp.dot(
        earlier[pl.ds(pl.multiple_of(me * tok, tok), tok), :], all_hot,
        preferred_element_type=jnp.float32,
    )
    own_inside = jnp.where(
        own_before < limit.astype(jnp.float32), hot[me].astype(jnp.float32), 0.0
    )
    own_text = jnp.dot(
        own_inside.astype(jnp.bfloat16), jnp.ones((LANES, LANES), jnp.bfloat16),
        preferred_element_type=jnp.float32,
    )
    own_code = 2.0 * own_id + jnp.where(own_text > 0.5, 0.0, 1.0)
    for tile in range(hidden_ref.shape[1] // LANES):
        cols = slice(tile * LANES, (tile + 1) * LANES)
        total = jnp.zeros((tok, LANES), jnp.float32)
        for r in range(requests):
            pair = gate_ref[r, :, cols].astype(jnp.float32)
            for s in range(2):
                total = jnp.where(own_code == float(2 * r + s), pair[s : s + 1], total)
        gate_rows[tile] = total

    for j in range(own_heads):
        settle(owned.at[j, :, chip, core], slot_sem.at[1 + j])
        settle(owned.at[j, 0:2, 0 : chips - 1], recv_sem.at[5 + 2 * j])
        beside[j].wait_recv()
        if j == 0:
            for to_chip in far_chips:
                remote(
                    shared_out.at[to_chip], back.at[chip * per_chip],
                    send_sem.at[2], recv_sem.at[2], to_chip * 2 + core,
                )
        query_n = normed(owned[j, 0], query_gains[...]).reshape(full)
        key_n = normed(owned[j, 1], key_gains[...]).reshape(full)
        weights[j] = attention_weights(query_n, key_n, bias[...].reshape(tokens, tokens))
    across = []
    for j in range(own_heads):
        settle(owned.at[j, 2, 0 : chips - 1], recv_sem.at[6 + 2 * j])
        owned_out[j] = jnp.dot(
            weights[j], owned[j, 2].reshape(full), preferred_element_type=jnp.float32
        ).astype(jnp.bfloat16).reshape(chips, 2, tok, HEAD_DIM)
        head = chip * per_chip + own_head(j, core)
        for to_chip in far_chips:
            for a_core in range(2):
                remote(
                    owned_out.at[j, to_chip, a_core], back.at[head],
                    send_sem.at[3], recv_sem.at[3 + core], to_chip * 2 + a_core,
                )
        across.append(remote(
            owned_out.at[j, chip, 1 - core], back.at[head],
            relay_send.at[3 + own_heads + j], relay_recv.at[3 + own_heads + j], partner,
        ))

    def finish(head):
        cols = slice(head * HEAD_DIM, (head + 1) * HEAD_DIM)
        out_ref[:, cols] = (
            hidden_ref[:, cols].astype(jnp.float32)
            + gate_rows[head] * back[head].astype(jnp.float32)
        ).astype(jnp.bfloat16)

    for copy in seg_copies + [seg_relay] + relays + beside:
        copy.wait_send()

    @pl.when(jnp.logical_not(inner))
    def _():
        for place in range(2):
            settle(shared_sends[place], send_sem.at[place])

    for j in range(own_heads):
        settle(owned.at[j, 0:2, 0 : chips - 1], send_sem.at[5 + 2 * j])
        settle(owned.at[j, 2, 0 : chips - 1], send_sem.at[6 + 2 * j])
    back[chip * per_chip] = shared_out[chip]
    settle(back.at[0 : chips - 1], recv_sem.at[2])
    for a_chip in range(chips):
        finish(a_chip * per_chip)
    for j in range(own_heads):
        back[chip * per_chip + own_head(j, core)] = owned_out.at[j, chip, core][...]
    for copy in across:
        copy.wait_recv()
    for a_core in FIRST_CORE:
        settle(back.at[0 : own_heads * (chips - 1)], recv_sem.at[3 + a_core])
        for a_chip in range(chips):
            for j in range(own_heads):
                finish(a_chip * per_chip + own_head(j, a_core))

    for copy in across:
        copy.wait_send()
    settle(back.at[0 : chips - 1], send_sem.at[2])
    settle(back.at[0 : 2 * own_heads * (chips - 1)], send_sem.at[3])


def fused(
    hidden, queries, key_rows, values, query_gain, key_gain, gate_table, segment, text_count
):
    devices = lax.axis_size("seq")
    chips = devices // 2
    tok, width = hidden.shape
    heads = width // HEAD_DIM
    own_heads = heads // chips // 2
    tokens = devices * tok
    hbm = pl.BlockSpec(memory_space=pl.ANY)
    block = (tok, HEAD_DIM)
    dma = pltpu.SemaphoreType.DMA
    return pl.pallas_call(
        functools.partial(fused_kernel, devices),
        out_shape=jax.ShapeDtypeStruct((tok, width), jnp.bfloat16),
        in_specs=[hbm] * 9,
        out_specs=pl.BlockSpec(memory_space=pltpu.VMEM),
        scratch_shapes=[
            pltpu.VMEM((1, text_count.shape[0]), jnp.int32),
            pltpu.VMEM(hidden.shape, hidden.dtype),
            pltpu.VMEM(query_gain.shape, query_gain.dtype),
            pltpu.VMEM(key_gain.shape, key_gain.dtype),
            pltpu.VMEM(gate_table.shape, gate_table.dtype),
            pltpu.VMEM((3, tok, width), jnp.bfloat16),
            pltpu.VMEM((3, chips, 2) + block, jnp.bfloat16),
            pltpu.VMEM((own_heads, 3, chips, 2) + block, jnp.bfloat16),
            pltpu.VMEM((own_heads, tokens, tokens), jnp.bfloat16),
            pltpu.VMEM((chips,) + block, jnp.bfloat16),
            pltpu.VMEM((own_heads, chips, 2) + block, jnp.bfloat16),
            pltpu.VMEM((heads,) + block, jnp.bfloat16),
            pltpu.VMEM((chips, 2, 1, tok), jnp.int32),
            pltpu.VMEM((devices, tok, LANES), jnp.bfloat16),
            pltpu.VMEM((tokens, tokens), jnp.bfloat16),
            pltpu.VMEM((chips, 2, tok, LANES), jnp.float32),
            pltpu.VMEM((chips, 2, tok, LANES), jnp.float32),
            pltpu.VMEM((chips, 2, tok, tokens), jnp.float32),
            pltpu.VMEM((heads, tok, LANES), jnp.float32),
            pltpu.SemaphoreType.REGULAR((devices,)),
            pltpu.SemaphoreType.REGULAR,
            dma((5,)),
            dma,
            dma((2,)),
            dma((1 + own_heads,)),
            dma((chips - 1,)),
            dma((chips,)),
            dma((5 + 2 * own_heads,)),
            dma((5 + 2 * own_heads,)),
            dma((3 + 2 * own_heads,)),
            dma((3 + 2 * own_heads,)),
        ],
        compiler_params=pltpu.CompilerParams(
            collective_id=0, has_side_effects=True, vmem_limit_bytes=16 * 1024 * 1024
        ),
    )(*(
        pltpu.with_memory_space_constraint(array, pltpu.HBM)
        for array in (
            segment.reshape(1, tok), queries, key_rows, values,
            text_count.reshape(1, -1), hidden, query_gain, key_gain, gate_table,
        )
    ))


def program(*arrays):
    devices = lax.axis_size("seq")
    tok, width = arrays[0].shape
    requests = arrays[-1].shape[0]
    whole_heads = devices % 8 == 0 and (width // HEAD_DIM) % (devices // 2) == 0
    odd = whole_heads and width // HEAD_DIM // (devices // 2) % 2 == 1
    if odd and devices * tok <= 512 and requests <= LANES and tok % 16 == 0:
        return fused(*arrays)
    return per_device(*arrays)


def solution(mesh):
    return jax.shard_map(
        program,
        mesh=mesh,
        in_specs=(
            P(("groups", "seq"), None),
            P(("groups", "seq"), None),
            P(("groups", "seq"), None),
            P(("groups", "seq"), None),
            P(),
            P(),
            P("groups", None, None),
            P(("groups", "seq")),
            P("groups"),
        ),
        out_specs=P(("groups", "seq"), None),
        check_vma=False,
    )
```

```python
import functools
import math

import jax
import jax.numpy as jnp
from jax import lax
from jax.experimental import pallas as pl
from jax.experimental.pallas import tpu as pltpu
from jax.sharding import PartitionSpec as P

HEAD_DIM = 128


EPSILON = 1e-06
MASKED = -1e30


def head_norm(rows_in, gains, stream):
    row_count = rows_in.shape[0]
    per_head = rows_in.astype(jnp.float32).reshape(row_count, -1, HEAD_DIM)
    inverse = lax.rsqrt(jnp.mean(per_head * per_head, axis=-1, keepdims=True) + EPSILON)
    gain_rows = jnp.where((stream == 0)[:, None], gains[0][None, :], gains[1][None, :])
    return (per_head * inverse * gain_rows[:, None, :]).astype(jnp.bfloat16).reshape(row_count, -1)


def attend(query_block, block_segment, key_data, value_data, key_segment):
    scores = jnp.einsum(
        "qhd,khd->hqk", query_block, key_data, preferred_element_type=jnp.float32
    ) * (1.0 / math.sqrt(HEAD_DIM))
    allowed = (block_segment[:, None] == key_segment[None, :])[None, :, :]
    scores = jnp.where(allowed, scores, MASKED)
    largest = jnp.max(scores, axis=-1, keepdims=True)
    weights = jnp.exp(scores - largest)
    weights = (weights / jnp.sum(weights, axis=-1, keepdims=True)).astype(jnp.bfloat16)
    return jnp.einsum(
        "hqk,khd->qhd", weights, value_data, preferred_element_type=jnp.float32
    ).astype(jnp.bfloat16)


def per_device(
    hidden, queries, key_rows, values, query_gain, key_gain, gate_table, segment, text_count
):
    tok_rows = hidden.shape[0]
    width_all = hidden.shape[1]
    devices = lax.axis_size("seq")
    requests = text_count.shape[0]
    seg_hot = (segment[:, None] == jnp.arange(requests, dtype=jnp.int32)[None, :]).astype(jnp.int32)
    local_counts = jnp.sum(seg_hot, axis=0)
    all_counts = lax.all_gather(local_counts[None, :], "seq", axis=0, tiled=True)
    lower_rows = (jnp.arange(devices, dtype=jnp.int32) < lax.axis_index("seq")).astype(jnp.int32)
    before = jnp.sum(all_counts * lower_rows[:, None], axis=0)
    position = jnp.sum((jnp.cumsum(seg_hot, axis=0) - seg_hot + before[None, :]) * seg_hot, axis=1)
    text_limit = jnp.sum(seg_hot * text_count[None, :], axis=1)
    stream = (position >= text_limit).astype(jnp.int32)
    query_normed = head_norm(queries, query_gain, stream)
    key_normed = head_norm(key_rows, key_gain, stream)
    groups = 8
    pair_merge = 2
    slices = devices // groups
    cap_rows = 4 * tok_rows // devices + max(1, tok_rows // devices)
    bucket_rows = cap_rows * pair_merge
    head_cols = width_all // groups
    owner_slice = segment // pair_merge
    owner_hot = (owner_slice[:, None] == jnp.arange(slices, dtype=jnp.int32)[None, :]).astype(
        jnp.int32
    )
    owner_rank = jnp.sum((jnp.cumsum(owner_hot, axis=0) - owner_hot) * owner_hot, axis=1)
    slot_place = owner_slice * bucket_rows + owner_rank
    bucket_index = (
        jnp.full((slices * bucket_rows,), tok_rows, jnp.int32)
        .at[slot_place]
        .set(jnp.arange(tok_rows, dtype=jnp.int32))
    )
    stacked = jnp.concatenate(
        [
            query_normed.reshape(tok_rows, groups, head_cols),
            key_normed.reshape(tok_rows, groups, head_cols),
            values.reshape(tok_rows, groups, head_cols),
        ],
        axis=2,
    ).transpose(1, 0, 2)
    outgoing = jnp.take(stacked, bucket_index, axis=1, mode="fill", fill_value=0).reshape(
        devices, bucket_rows, 3 * head_cols
    )
    slot_segment = jnp.take(segment, bucket_index, axis=0, mode="fill", fill_value=-1)
    segment_out = jnp.broadcast_to(slot_segment[None, :], (groups, slices * bucket_rows)).reshape(
        devices, bucket_rows
    )
    arrived, arrived_segment = (
        lax.all_to_all(outgoing, "seq", split_axis=0, concat_axis=0, tiled=True),
        lax.all_to_all(segment_out, "seq", split_axis=0, concat_axis=0, tiled=True),
    )
    slot_count = devices * bucket_rows
    per_head = head_cols // HEAD_DIM
    slot_data = arrived.reshape(slot_count, 3 * head_cols)
    query_all = slot_data[:, :head_cols].reshape(slot_count, per_head, HEAD_DIM)
    key_all = slot_data[:, head_cols : 2 * head_cols].reshape(slot_count, per_head, HEAD_DIM)
    value_all = slot_data[:, 2 * head_cols :].reshape(slot_count, per_head, HEAD_DIM)
    key_segment = arrived_segment.reshape(slot_count)
    if slot_count % 512 == 0:
        block_rows = 512
    elif slot_count % 256 == 0:
        block_rows = 256
    else:
        block_rows = slot_count

    def one_block(first_row):
        return attend(query_all, key_segment, key_all, value_all, key_segment)

    results = lax.map(one_block, jnp.arange(slot_count // block_rows, dtype=jnp.int32) * block_rows)
    returning = results.reshape(devices, bucket_rows, head_cols)
    returned = lax.all_to_all(returning, "seq", split_axis=0, concat_axis=0, tiled=True)
    returned = returned.reshape(groups, slices * bucket_rows, head_cols)
    attention = (
        jnp.take(returned, slot_place, axis=1).transpose(1, 0, 2).reshape(tok_rows, width_all)
    )
    gate_rows = jnp.take(gate_table.reshape(requests * 2, width_all), segment * 2 + stream, axis=0)
    mixed = hidden.astype(jnp.float32) + gate_rows.astype(jnp.float32) * attention.astype(
        jnp.float32
    )
    return mixed.astype(jnp.bfloat16)


LANES = 128
CONTRACT_LAST = (((1,), (1,)), ((), ()))


def normed(rows, gain_rows):
    wide = rows.astype(jnp.float32)
    inverse = lax.rsqrt(jnp.mean(wide * wide, axis=-1, keepdims=True) + EPSILON)
    return (wide * inverse * gain_rows).astype(jnp.bfloat16)


def fused_kernel(
    devices, segment_hbm, query_hbm, key_hbm, value_hbm,
    text_hbm, hidden_hbm, query_gain_hbm, key_gain_hbm, gate_hbm, out_ref,
    text_ref, hidden_ref, query_gain_ref, key_gain_ref, gate_ref,
    staged, shared, owned, shared_out, owned_out, back, seg_all, hot, earlier,
    query_gains, key_gains, bias, gate_rows,
    here_sem, go_sem, load_sem, seg_own_sem, stage_sem, slot_sem,
    seg_recv, send_sem, recv_sem, relay_recv,
):
    chips = devices // 2
    levels = chips // 2
    tok = hidden_hbm.shape[0]
    per_chip = hidden_hbm.shape[1] // HEAD_DIM // chips
    own_heads = per_chip // 2
    requests = gate_hbm.shape[0]
    tokens = devices * tok
    me = lax.axis_index("seq")
    chip, core = me // 2, me % 2
    row, level = chip % 2, chip // 2
    partner = me + 1 - 2 * core
    sources = (query_hbm, key_hbm, value_hbm)

    def columns(head):
        return pl.ds(pl.multiple_of(head * HEAD_DIM, HEAD_DIM), HEAD_DIM)

    def chip_at(a_level, a_row):
        return a_level * 2 + a_row

    def signal(semaphore, device):
        pl.semaphore_signal(
            semaphore, inc=1, device_id={"seq": device}, device_id_type=pl.DeviceIdType.MESH
        )

    def remote(src, dst, send, recv, device):
        copy = pltpu.make_async_remote_copy(
            src_ref=src, dst_ref=dst, send_sem=send, recv_sem=recv,
            device_id={"seq": device}, device_id_type=pl.DeviceIdType.MESH,
        )
        copy.start()
        return copy

    def settle(ref, semaphore):
        pltpu.make_async_copy(ref, ref, semaphore).wait()

    toward = 1 - 2 * (level // (levels // 2))
    near_first = [(level + levels + toward * step) % levels for step in range(1, levels)]
    far_first = [(level + levels - toward * step) % levels for step in range(1, levels)]
    orders = []
    for start in range(levels):
        first = start + (1 if start < levels // 2 else -1)
        rest = list(range(start - 1, -1, -1)) + list(range(start + 1, levels))
        orders.append([first] + [n for n in rest if n != first])

    def pick(values):
        result = values[0]
        for start in range(1, levels):
            result = jnp.where(level == start, values[start], result)
        return result

    met = [pick([order[place] for order in orders]) for place in range(levels - 1)]
    near_chips = []
    for place, a_level in enumerate(near_first):
        near_chips.append(chip_at(a_level, row))
        near_chips.append(chip_at(a_level, 1 - row))
    near_chips.append(chip_at(level, 1 - row))
    far_chips = []
    for a_level in far_first:
        far_chips += [chip_at(a_level, 0), chip_at(a_level, 1)]
    far_chips.append(chip_at(level, 1 - row))

    for part, source in enumerate(sources):
        pltpu.make_async_copy(source, staged.at[part], stage_sem).start()

    barrier = pltpu.get_barrier_semaphore()

    @pl.when(me > 0)
    def _():
        pl.semaphore_wait(barrier, (level + levels - 1) // levels + row + core)

    @pl.when(level + 1 < levels)
    def _():
        signal(barrier, me + 4)

    @pl.when(row == 0)
    def _():
        signal(barrier, me + 2)

    @pl.when(core == 0)
    def _():
        signal(barrier, me + 1)

    for down in range(levels):
        for row_down in range(2):
            for core_down in range(2):
                if down + row_down + core_down > 0:
                    fits = level >= down
                    if row_down:
                        fits = jnp.logical_and(fits, row == 1)
                    if core_down:
                        fits = jnp.logical_and(fits, core == 1)

                    @pl.when(fits)
                    def _():
                        signal(here_sem.at[me], me - 4 * down - 2 * row_down - core_down)

    def vouched(condition, a_level, a_row, a_core):
        @pl.when(condition)
        def _():
            pl.semaphore_wait(here_sem.at[chip_at(a_level, a_row) * 2 + a_core], 1)

    seg_own = pltpu.make_async_copy(segment_hbm, seg_all.at[chip, core], seg_own_sem)
    seg_own.start()
    for part, source in enumerate(sources):
        pltpu.make_async_copy(
            source.at[:, columns(chip * per_chip)], shared.at[part, chip, core], slot_sem
        ).start()
        for j in range(own_heads):
            pltpu.make_async_copy(
                source.at[:, columns(chip * per_chip + 1 + core * own_heads + j)],
                owned.at[j, part, me], slot_sem,
            ).start()
    loads = [
        pltpu.make_async_copy(source, target, load_sem.at[place])
        for place, (source, target) in enumerate(
            (
                (text_hbm, text_ref), (query_gain_hbm, query_gain_ref),
                (key_gain_hbm, key_gain_ref), (gate_hbm, gate_ref), (hidden_hbm, hidden_ref),
            )
        )
    ]
    for copy in loads:
        copy.start()
    settle(staged, stage_sem)
    seg_own.wait()

    def own_head(j, a_core):
        return 1 + a_core * own_heads + j

    def send_owned(to_chip, a_core):
        for j in range(own_heads):
            remote(
                staged.at[:, :, columns(to_chip * per_chip + own_head(j, a_core))],
                owned.at[j, :, me], send_sem.at[1], recv_sem.at[2 + j], to_chip * 2 + a_core,
            )

    def send_shared(to_chip):
        device = to_chip * 2 + core
        own_ids = seg_all.at[chip, core]
        remote(own_ids, own_ids, send_sem.at[0], seg_recv, device)
        remote(
            staged.at[:, :, columns(to_chip * per_chip)], shared.at[:, chip, core],
            send_sem.at[0], recv_sem.at[0], device,
        )

    low = core == 0
    upper = row == 0
    low_upper = jnp.logical_and(low, upper)

    for place, a_level in enumerate(met):
        above = a_level > level
        vouched(above, a_level, row, core)
        send_shared(chip_at(a_level, row))
        if place == 0:
            @pl.when(low)
            def _():
                send_owned(chip_at(met[0], row), 0)

            vouched(low, level, row, 1)
            vouched(jnp.logical_and(low, above), a_level, row, 1)

            @pl.when(jnp.logical_not(low))
            def _():
                send_owned(chip_at(met[0], row), 0)

            continue
        if place == 1:
            vouched(upper, level, 1, core)
            send_shared(chip_at(level, 1 - row))
            vouched(jnp.logical_and(met[0] > level, upper), met[0], 1, core)
            send_shared(chip_at(met[0], 1 - row))
        vouched(jnp.logical_and(above, upper), a_level, 1, core)
        send_shared(chip_at(a_level, 1 - row))

    send_owned(chip, 1 - core)
    vouched(low_upper, level, 1, 1)
    vouched(jnp.logical_and(low_upper, met[0] > level), met[0], 1, 1)
    for a_level in met[1:]:
        vouched(jnp.logical_and(low, a_level > level), a_level, row, 1)
        vouched(jnp.logical_and(low_upper, a_level > level), a_level, 1, 1)

    far_pairs = [(chip_at(a_level, 1 - row), chip_at(a_level, row)) for a_level in far_first]
    next_door = chip_at(level, 1 - row)
    across_chips = [to_chip for pair in far_pairs[:-1] for to_chip in pair]

    def send_all_owned(to_chips, last_chips):
        for to_chip in to_chips:
            send_owned(to_chip, 0)
        for to_chip in to_chips + last_chips:
            send_owned(to_chip, 1)

    inner = jnp.logical_or(level == levels // 2 - 1, level == levels // 2)

    @pl.when(inner)
    def _():
        send_all_owned(across_chips + [far_pairs[-1][0], next_door], [far_pairs[-1][1]])

    earlier[...] = (
        lax.broadcasted_iota(jnp.int32, (tokens, tokens), 1)
        < lax.broadcasted_iota(jnp.int32, (tokens, tokens), 0)
    ).astype(jnp.float32).astype(jnp.bfloat16)

    def settle_shared_sends():
        settle(shared.at[:, 0 : chips - 1, 0], send_sem.at[0])
        settle(seg_all.at[0 : chips - 1, 0], send_sem.at[0])

    lower = level < levels // 2
    outer = jnp.logical_not(inner)
    lower_outer = jnp.logical_and(lower, outer)

    @pl.when(outer)
    def _():
        send_all_owned([far_pairs[-1][0], next_door], [far_pairs[-1][1]])

    @pl.when(jnp.logical_not(lower_outer))
    def _():
        settle_shared_sends()

    @pl.when(jnp.logical_and(lower, inner))
    def _():
        for step in range(1, levels // 2):
            signal(go_sem, chip_at(level - step, row) * 2 + core)

    @pl.when(lower_outer)
    def _():
        pl.semaphore_wait(go_sem, 1)

    @pl.when(outer)
    def _():
        send_all_owned(across_chips, [])

    settle(seg_all.at[0 : chips - 1, 0], seg_recv)
    relays = [remote(
        seg_all.at[:, core], seg_all.at[:, core], send_sem.at[1], relay_recv.at[0], partner
    )]
    settle(owned.at[0, :, 0 : 1 + own_heads], slot_sem)
    settle(shared.at[:, 0 : chips - 1, 0], recv_sem.at[0])
    relays.append(remote(
        shared.at[1:3, :, core], shared.at[1:3, :, core], send_sem.at[1], relay_recv.at[1], partner
    ))
    for copy in loads:
        copy.wait()
    relays[0].wait_recv()
    eye = (
        lax.broadcasted_iota(jnp.int32, (tok, tok), 0)
        == lax.broadcasted_iota(jnp.int32, (tok, tok), 1)
    ).astype(jnp.float32).astype(jnp.bfloat16)
    ids = lax.broadcasted_iota(jnp.int32, (LANES, tok), 0)
    for n in range(devices):
        flipped = (ids == seg_all[n // 2, n % 2]).astype(jnp.float32).astype(jnp.bfloat16)
        hot[n] = lax.dot_general(
            eye, flipped, CONTRACT_LAST, preferred_element_type=jnp.float32
        ).astype(jnp.bfloat16)
    all_hot = hot[...].reshape(tokens, LANES)
    before = jnp.dot(earlier[...], all_hot, preferred_element_type=jnp.float32)
    lane = lax.broadcasted_iota(jnp.int32, (1, LANES), 1)
    limit = jnp.zeros((1, LANES), jnp.int32)
    for r in range(requests):
        limit = jnp.where(lane == r, text_ref[0:1, r : r + 1], limit)
    inside = jnp.where(before < limit.astype(jnp.float32), all_hot.astype(jnp.float32), 0.0)
    text = jnp.dot(
        inside.astype(jnp.bfloat16), jnp.ones((LANES, LANES), jnp.bfloat16),
        preferred_element_type=jnp.float32,
    ) > 0.5
    query_gain, key_gain = query_gain_ref[...], key_gain_ref[...]
    spread = (chips, 2, tok, LANES)
    query_gains[...] = jnp.where(text, query_gain[0:1], query_gain[1:2]).reshape(spread)
    key_gains[...] = jnp.where(text, key_gain[0:1], key_gain[1:2]).reshape(spread)
    same = lax.dot_general(all_hot, all_hot, CONTRACT_LAST, preferred_element_type=jnp.float32)
    bias[...] = jnp.where(same > 0.5, 0.0, MASKED).reshape(chips, 2, tok, tokens)

    scale = 1.0 / math.sqrt(HEAD_DIM)

    def attention_weights(query_n, key_n, query_bias):
        scores = lax.dot_general(
            query_n, key_n, CONTRACT_LAST, preferred_element_type=jnp.float32
        ) * scale + query_bias
        grown = jnp.exp(scores - jnp.max(scores, axis=-1, keepdims=True))
        return (grown * (1.0 / jnp.sum(grown, axis=-1, keepdims=True))).astype(jnp.bfloat16)

    half = (tokens // 2, HEAD_DIM)
    full = (tokens, HEAD_DIM)
    query_n = normed(shared.at[0, :, core][...], query_gains.at[:, core][...]).reshape(half)
    relays[1].wait_recv()
    key_n = normed(shared[1], key_gains[...]).reshape(full)
    part_weights = attention_weights(
        query_n, key_n, bias.at[:, core][...].reshape(tokens // 2, tokens)
    )
    shared_out[...] = jnp.dot(
        part_weights, shared[2].reshape(full), preferred_element_type=jnp.float32
    ).astype(jnp.bfloat16).reshape(chips, tok, HEAD_DIM)

    number = lax.broadcasted_iota(jnp.int32, (LANES, LANES), 0).astype(jnp.float32)
    own_id = jnp.dot(hot[me], number.astype(jnp.bfloat16), preferred_element_type=jnp.float32)
    own_before = jnp.dot(
        earlier[pl.ds(pl.multiple_of(me * tok, tok), tok), :], all_hot,
        preferred_element_type=jnp.float32,
    )
    own_inside = jnp.where(
        own_before < limit.astype(jnp.float32), hot[me].astype(jnp.float32), 0.0
    )
    own_text = jnp.dot(
        own_inside.astype(jnp.bfloat16), jnp.ones((LANES, LANES), jnp.bfloat16),
        preferred_element_type=jnp.float32,
    )
    own_code = 2.0 * own_id + jnp.where(own_text > 0.5, 0.0, 1.0)
    for tile in range(hidden_ref.shape[1] // LANES):
        cols = slice(tile * LANES, (tile + 1) * LANES)
        total = jnp.zeros((tok, LANES), jnp.float32)
        for r in range(requests):
            pair = gate_ref[r, :, cols].astype(jnp.float32)
            for s in range(2):
                total = jnp.where(own_code == float(2 * r + s), pair[s : s + 1], total)
        gate_rows[tile] = total

    far_half = 1 - level // (levels // 2)
    for j in range(own_heads):
        settle(owned.at[j, :, 0 : devices - 1], recv_sem.at[2 + j])
        if j == 0:
            for to_chip in far_chips:
                remote(
                    shared_out.at[to_chip], back.at[chip * per_chip],
                    send_sem.at[1], recv_sem.at[1], to_chip * 2 + core,
                )
        flat = (devices, tok, LANES)
        key_n = normed(owned[j, 1], key_gains[...].reshape(flat)).reshape(full)
        value_all = owned[j, 2].reshape(full)
        head = chip * per_chip + own_head(j, core)
        for part in (far_half, 1 - far_half):
            chip_rows = pl.ds(part * (chips // 2), chips // 2)
            rows_in = owned.at[j, 0, pl.ds(part * chips, chips)][...]
            gain_rows = query_gains.at[chip_rows][...].reshape(chips, tok, LANES)
            bias_rows = bias.at[chip_rows][...].reshape(tokens // 2, tokens)
            part_weights = attention_weights(normed(rows_in, gain_rows).reshape(half), key_n, bias_rows)
            owned_out[j, chip_rows] = jnp.dot(
                part_weights, value_all, preferred_element_type=jnp.float32
            ).astype(jnp.bfloat16).reshape(chips // 2, 2, tok, HEAD_DIM)
            for to_chip in far_chips:
                @pl.when(jnp.logical_and(to_chip // (chips // 2) == part, to_chip != chip))
                def _():
                    for a_core in range(2):
                        remote(
                            owned_out.at[j, to_chip, a_core], back.at[head],
                            send_sem.at[1], recv_sem.at[1], to_chip * 2 + a_core,
                        )
        remote(
            owned_out.at[j, chip, 1 - core], back.at[head],
            send_sem.at[1], recv_sem.at[1], partner,
        )

    def finish(head):
        cols = slice(head * HEAD_DIM, (head + 1) * HEAD_DIM)
        out_ref[:, cols] = (
            hidden_ref[:, cols].astype(jnp.float32)
            + gate_rows[head] * back[head].astype(jnp.float32)
        ).astype(jnp.bfloat16)

    @pl.when(lower_outer)
    def _():
        settle_shared_sends()

    settle(seg_all.at[:, core], send_sem.at[1])
    settle(shared.at[1:3, :, core], send_sem.at[1])
    for j in range(own_heads):
        settle(owned.at[j, :, 0 : devices - 1], send_sem.at[1])
    results = back.at[0 : per_chip * (chips - 1) + own_heads]
    settle(results, send_sem.at[1])
    back[chip * per_chip] = shared_out[chip]
    for j in range(own_heads):
        back[chip * per_chip + own_head(j, core)] = owned_out.at[j, chip, core][...]
    settle(results, recv_sem.at[1])
    for head in range(chips * per_chip):
        finish(head)


def fused(
    hidden, queries, key_rows, values, query_gain, key_gain, gate_table, segment, text_count
):
    devices = lax.axis_size("seq")
    chips = devices // 2
    tok, width = hidden.shape
    heads = width // HEAD_DIM
    own_heads = heads // chips // 2
    tokens = devices * tok
    hbm = pl.BlockSpec(memory_space=pl.ANY)
    block = (tok, HEAD_DIM)
    dma = pltpu.SemaphoreType.DMA
    return pl.pallas_call(
        functools.partial(fused_kernel, devices),
        out_shape=jax.ShapeDtypeStruct((tok, width), jnp.bfloat16),
        in_specs=[hbm] * 9,
        out_specs=pl.BlockSpec(memory_space=pltpu.VMEM),
        scratch_shapes=[
            pltpu.VMEM((1, text_count.shape[0]), jnp.int32),
            pltpu.VMEM(hidden.shape, hidden.dtype),
            pltpu.VMEM(query_gain.shape, query_gain.dtype),
            pltpu.VMEM(key_gain.shape, key_gain.dtype),
            pltpu.VMEM(gate_table.shape, gate_table.dtype),
            pltpu.VMEM((3, tok, width), jnp.bfloat16),
            pltpu.VMEM((3, chips, 2) + block, jnp.bfloat16),
            pltpu.VMEM((own_heads, 3, devices) + block, jnp.bfloat16),
            pltpu.VMEM((chips,) + block, jnp.bfloat16),
            pltpu.VMEM((own_heads, chips, 2) + block, jnp.bfloat16),
            pltpu.VMEM((heads,) + block, jnp.bfloat16),
            pltpu.VMEM((chips, 2, 1, tok), jnp.int32),
            pltpu.VMEM((devices, tok, LANES), jnp.bfloat16),
            pltpu.VMEM((tokens, tokens), jnp.bfloat16),
            pltpu.VMEM((chips, 2, tok, LANES), jnp.float32),
            pltpu.VMEM((chips, 2, tok, LANES), jnp.float32),
            pltpu.VMEM((chips, 2, tok, tokens), jnp.float32),
            pltpu.VMEM((heads, tok, LANES), jnp.float32),
            pltpu.SemaphoreType.REGULAR((devices,)),
            pltpu.SemaphoreType.REGULAR,
            dma((5,)),
            dma,
            dma,
            dma,
            dma,
            dma((2,)),
            dma((2 + own_heads,)),
            dma((2,)),
        ],
        compiler_params=pltpu.CompilerParams(
            collective_id=0, has_side_effects=True, vmem_limit_bytes=16 * 1024 * 1024
        ),
    )(*(
        pltpu.with_memory_space_constraint(array, pltpu.HBM)
        for array in (
            segment.reshape(1, tok), queries, key_rows, values,
            text_count.reshape(1, -1), hidden, query_gain, key_gain, gate_table,
        )
    ))


def program(*arrays):
    devices = lax.axis_size("seq")
    tok, width = arrays[0].shape
    requests = arrays[-1].shape[0]
    whole_heads = devices % 8 == 0 and (width // HEAD_DIM) % (devices // 2) == 0
    odd = whole_heads and width // HEAD_DIM // (devices // 2) % 2 == 1
    if odd and devices * tok <= 512 and requests <= LANES and tok % 16 == 0:
        return fused(*arrays)
    return per_device(*arrays)


def solution(mesh):
    return jax.shard_map(
        program,
        mesh=mesh,
        in_specs=(
            P(("groups", "seq"), None),
            P(("groups", "seq"), None),
            P(("groups", "seq"), None),
            P(("groups", "seq"), None),
            P(),
            P(),
            P("groups", None, None),
            P(("groups", "seq")),
            P("groups"),
        ),
        out_specs=P(("groups", "seq"), None),
        check_vma=False,
    )
```

```python
import functools
import math

import jax
import jax.numpy as jnp
from jax import lax
from jax.experimental import pallas as pl
from jax.experimental.pallas import tpu as pltpu
from jax.sharding import PartitionSpec as P

HEAD_DIM = 128


EPSILON = 1e-06
MASKED = -1e30


def head_norm(rows_in, gains, stream):
    row_count = rows_in.shape[0]
    per_head = rows_in.astype(jnp.float32).reshape(row_count, -1, HEAD_DIM)
    inverse = lax.rsqrt(jnp.mean(per_head * per_head, axis=-1, keepdims=True) + EPSILON)
    gain_rows = jnp.where((stream == 0)[:, None], gains[0][None, :], gains[1][None, :])
    return (per_head * inverse * gain_rows[:, None, :]).astype(jnp.bfloat16).reshape(row_count, -1)


def attend(query_block, block_segment, key_data, value_data, key_segment):
    scores = jnp.einsum(
        "qhd,khd->hqk", query_block, key_data, preferred_element_type=jnp.float32
    ) * (1.0 / math.sqrt(HEAD_DIM))
    allowed = (block_segment[:, None] == key_segment[None, :])[None, :, :]
    scores = jnp.where(allowed, scores, MASKED)
    largest = jnp.max(scores, axis=-1, keepdims=True)
    weights = jnp.exp(scores - largest)
    weights = (weights / jnp.sum(weights, axis=-1, keepdims=True)).astype(jnp.bfloat16)
    return jnp.einsum(
        "hqk,khd->qhd", weights, value_data, preferred_element_type=jnp.float32
    ).astype(jnp.bfloat16)


def per_device(
    hidden, queries, key_rows, values, query_gain, key_gain, gate_table, segment, text_count
):
    tok_rows = hidden.shape[0]
    width_all = hidden.shape[1]
    devices = lax.axis_size("seq")
    requests = text_count.shape[0]
    seg_hot = (segment[:, None] == jnp.arange(requests, dtype=jnp.int32)[None, :]).astype(jnp.int32)
    local_counts = jnp.sum(seg_hot, axis=0)
    all_counts = lax.all_gather(local_counts[None, :], "seq", axis=0, tiled=True)
    lower_rows = (jnp.arange(devices, dtype=jnp.int32) < lax.axis_index("seq")).astype(jnp.int32)
    before = jnp.sum(all_counts * lower_rows[:, None], axis=0)
    position = jnp.sum((jnp.cumsum(seg_hot, axis=0) - seg_hot + before[None, :]) * seg_hot, axis=1)
    text_limit = jnp.sum(seg_hot * text_count[None, :], axis=1)
    stream = (position >= text_limit).astype(jnp.int32)
    query_normed = head_norm(queries, query_gain, stream)
    key_normed = head_norm(key_rows, key_gain, stream)
    groups = 8
    pair_merge = 2
    slices = devices // groups
    cap_rows = 4 * tok_rows // devices + max(1, tok_rows // devices)
    bucket_rows = cap_rows * pair_merge
    head_cols = width_all // groups
    owner_slice = segment // pair_merge
    owner_hot = (owner_slice[:, None] == jnp.arange(slices, dtype=jnp.int32)[None, :]).astype(
        jnp.int32
    )
    owner_rank = jnp.sum((jnp.cumsum(owner_hot, axis=0) - owner_hot) * owner_hot, axis=1)
    slot_place = owner_slice * bucket_rows + owner_rank
    bucket_index = (
        jnp.full((slices * bucket_rows,), tok_rows, jnp.int32)
        .at[slot_place]
        .set(jnp.arange(tok_rows, dtype=jnp.int32))
    )
    stacked = jnp.concatenate(
        [
            query_normed.reshape(tok_rows, groups, head_cols),
            key_normed.reshape(tok_rows, groups, head_cols),
            values.reshape(tok_rows, groups, head_cols),
        ],
        axis=2,
    ).transpose(1, 0, 2)
    outgoing = jnp.take(stacked, bucket_index, axis=1, mode="fill", fill_value=0).reshape(
        devices, bucket_rows, 3 * head_cols
    )
    slot_segment = jnp.take(segment, bucket_index, axis=0, mode="fill", fill_value=-1)
    segment_out = jnp.broadcast_to(slot_segment[None, :], (groups, slices * bucket_rows)).reshape(
        devices, bucket_rows
    )
    arrived, arrived_segment = (
        lax.all_to_all(outgoing, "seq", split_axis=0, concat_axis=0, tiled=True),
        lax.all_to_all(segment_out, "seq", split_axis=0, concat_axis=0, tiled=True),
    )
    slot_count = devices * bucket_rows
    per_head = head_cols // HEAD_DIM
    slot_data = arrived.reshape(slot_count, 3 * head_cols)
    query_all = slot_data[:, :head_cols].reshape(slot_count, per_head, HEAD_DIM)
    key_all = slot_data[:, head_cols : 2 * head_cols].reshape(slot_count, per_head, HEAD_DIM)
    value_all = slot_data[:, 2 * head_cols :].reshape(slot_count, per_head, HEAD_DIM)
    key_segment = arrived_segment.reshape(slot_count)
    if slot_count % 512 == 0:
        block_rows = 512
    elif slot_count % 256 == 0:
        block_rows = 256
    else:
        block_rows = slot_count

    def one_block(first_row):
        return attend(query_all, key_segment, key_all, value_all, key_segment)

    results = lax.map(one_block, jnp.arange(slot_count // block_rows, dtype=jnp.int32) * block_rows)
    returning = results.reshape(devices, bucket_rows, head_cols)
    returned = lax.all_to_all(returning, "seq", split_axis=0, concat_axis=0, tiled=True)
    returned = returned.reshape(groups, slices * bucket_rows, head_cols)
    attention = (
        jnp.take(returned, slot_place, axis=1).transpose(1, 0, 2).reshape(tok_rows, width_all)
    )
    gate_rows = jnp.take(gate_table.reshape(requests * 2, width_all), segment * 2 + stream, axis=0)
    mixed = hidden.astype(jnp.float32) + gate_rows.astype(jnp.float32) * attention.astype(
        jnp.float32
    )
    return mixed.astype(jnp.bfloat16)


LANES = 128
CONTRACT_LAST = (((1,), (1,)), ((), ()))


def normed(rows, gain_rows):
    wide = rows.astype(jnp.float32)
    inverse = lax.rsqrt(jnp.mean(wide * wide, axis=-1, keepdims=True) + EPSILON)
    return (wide * inverse * gain_rows).astype(jnp.bfloat16)


def fused_kernel(
    devices, segment_hbm, query_hbm, key_hbm, value_hbm,
    text_hbm, hidden_hbm, query_gain_hbm, key_gain_hbm, gate_hbm, out_ref,
    text_ref, hidden_ref, query_gain_ref, key_gain_ref, gate_ref,
    staged, shared, owned, shared_out, owned_out, back, seg_all, hot, earlier,
    query_gains, key_gains, bias, gate_rows,
    here_sem, go_sem, done_sem, load_sem, seg_own_sem, stage_sem, slot_sem,
    seg_recv, send_sem, recv_sem, relay_recv,
):
    chips = devices // 2
    levels = chips // 2
    tok = hidden_hbm.shape[0]
    per_chip = hidden_hbm.shape[1] // HEAD_DIM // chips
    own_heads = per_chip // 2
    requests = gate_hbm.shape[0]
    tokens = devices * tok
    me = lax.axis_index("seq")
    chip, core = me // 2, me % 2
    row, level = chip % 2, chip // 2
    partner = me + 1 - 2 * core
    sources = (query_hbm, key_hbm, value_hbm)

    def columns(head):
        return pl.ds(pl.multiple_of(head * HEAD_DIM, HEAD_DIM), HEAD_DIM)

    def chip_at(a_level, a_row):
        return a_level * 2 + a_row

    def signal(semaphore, device):
        pl.semaphore_signal(
            semaphore, inc=1, device_id={"seq": device}, device_id_type=pl.DeviceIdType.MESH
        )

    def remote(src, dst, send, recv, device):
        copy = pltpu.make_async_remote_copy(
            src_ref=src, dst_ref=dst, send_sem=send, recv_sem=recv,
            device_id={"seq": device}, device_id_type=pl.DeviceIdType.MESH,
        )
        copy.start()
        return copy

    def settle(ref, semaphore):
        pltpu.make_async_copy(ref, ref, semaphore).wait()

    toward = 1 - 2 * (level // (levels // 2))
    near_first = [(level + levels + toward * step) % levels for step in range(1, levels)]
    far_first = [(level + levels - toward * step) % levels for step in range(1, levels)]
    orders = []
    for start in range(levels):
        first = start + (1 if start < levels // 2 else -1)
        rest = list(range(start - 1, -1, -1)) + list(range(start + 1, levels))
        orders.append([first] + [n for n in rest if n != first])

    def pick(values):
        result = values[0]
        for start in range(1, levels):
            result = jnp.where(level == start, values[start], result)
        return result

    met = [pick([order[place] for order in orders]) for place in range(levels - 1)]
    near_chips = []
    for place, a_level in enumerate(near_first):
        near_chips.append(chip_at(a_level, row))
        near_chips.append(chip_at(a_level, 1 - row))
    near_chips.append(chip_at(level, 1 - row))
    far_chips = []
    for a_level in far_first:
        far_chips += [chip_at(a_level, 0), chip_at(a_level, 1)]
    far_chips.append(chip_at(level, 1 - row))

    for part, source in enumerate(sources):
        pltpu.make_async_copy(source, staged.at[part], stage_sem).start()

    barrier = pltpu.get_barrier_semaphore()

    @pl.when(me > 0)
    def _():
        pl.semaphore_wait(barrier, (level + levels - 1) // levels + row + core)

    @pl.when(level + 1 < levels)
    def _():
        signal(barrier, me + 4)

    @pl.when(row == 0)
    def _():
        signal(barrier, me + 2)

    @pl.when(core == 0)
    def _():
        signal(barrier, me + 1)

    for down in range(levels):
        for row_down in range(2):
            for core_down in range(2):
                if down + row_down + core_down > 0:
                    fits = level >= down
                    if row_down:
                        fits = jnp.logical_and(fits, row == 1)
                    if core_down:
                        fits = jnp.logical_and(fits, core == 1)

                    @pl.when(fits)
                    def _():
                        signal(here_sem.at[me], me - 4 * down - 2 * row_down - core_down)

    def vouched(condition, a_level, a_row, a_core):
        @pl.when(condition)
        def _():
            pl.semaphore_wait(here_sem.at[chip_at(a_level, a_row) * 2 + a_core], 1)

    seg_own = pltpu.make_async_copy(segment_hbm, seg_all.at[chip, core], seg_own_sem)
    seg_own.start()
    for part, source in enumerate(sources):
        pltpu.make_async_copy(
            source.at[:, columns(chip * per_chip)], shared.at[part, chip, core], slot_sem
        ).start()
        for j in range(own_heads):
            pltpu.make_async_copy(
                source.at[:, columns(chip * per_chip + 1 + core * own_heads + j)],
                owned.at[j, part, me], slot_sem,
            ).start()
    loads = [
        pltpu.make_async_copy(source, target, load_sem.at[place])
        for place, (source, target) in enumerate(
            (
                (text_hbm, text_ref), (query_gain_hbm, query_gain_ref),
                (key_gain_hbm, key_gain_ref), (gate_hbm, gate_ref), (hidden_hbm, hidden_ref),
            )
        )
    ]
    for copy in loads:
        copy.start()
    settle(staged, stage_sem)
    seg_own.wait()

    def own_head(j, a_core):
        return 1 + a_core * own_heads + j

    def send_owned(to_chip, a_core):
        for j in range(own_heads):
            remote(
                staged.at[:, :, columns(to_chip * per_chip + own_head(j, a_core))],
                owned.at[j, :, me], send_sem.at[1], recv_sem.at[2 + j], to_chip * 2 + a_core,
            )

    def send_shared(to_chip):
        device = to_chip * 2 + core
        own_ids = seg_all.at[chip, core]
        remote(own_ids, own_ids, send_sem.at[0], seg_recv, device)
        remote(
            staged.at[:, :, columns(to_chip * per_chip)], shared.at[:, chip, core],
            send_sem.at[0], recv_sem.at[0], device,
        )

    low = core == 0
    upper = row == 0
    low_upper = jnp.logical_and(low, upper)

    for place, a_level in enumerate(met):
        above = a_level > level
        vouched(above, a_level, row, core)
        send_shared(chip_at(a_level, row))
        if place == 0:
            @pl.when(low)
            def _():
                send_owned(chip_at(met[0], row), 0)

            vouched(low, level, row, 1)
            vouched(jnp.logical_and(low, above), a_level, row, 1)

            @pl.when(jnp.logical_not(low))
            def _():
                send_owned(chip_at(met[0], row), 0)

            continue
        if place == 1:
            vouched(upper, level, 1, core)
            send_shared(chip_at(level, 1 - row))
            vouched(jnp.logical_and(met[0] > level, upper), met[0], 1, core)
            send_shared(chip_at(met[0], 1 - row))
        vouched(jnp.logical_and(above, upper), a_level, 1, core)
        send_shared(chip_at(a_level, 1 - row))

    send_owned(chip, 1 - core)
    vouched(low_upper, level, 1, 1)
    vouched(jnp.logical_and(low_upper, met[0] > level), met[0], 1, 1)
    for a_level in met[1:]:
        vouched(jnp.logical_and(low, a_level > level), a_level, row, 1)
        vouched(jnp.logical_and(low_upper, a_level > level), a_level, 1, 1)

    far_pairs = [(chip_at(a_level, 1 - row), chip_at(a_level, row)) for a_level in far_first]
    next_door = chip_at(level, 1 - row)
    across_chips = [to_chip for pair in far_pairs[:-1] for to_chip in pair]

    def send_all_owned(to_chips, last_chips):
        for to_chip in to_chips:
            send_owned(to_chip, 0)
        for to_chip in to_chips + last_chips:
            send_owned(to_chip, 1)

    inner = jnp.logical_or(level == levels // 2 - 1, level == levels // 2)

    @pl.when(inner)
    def _():
        send_all_owned(across_chips + [far_pairs[-1][0], next_door], [far_pairs[-1][1]])

    earlier[...] = (
        lax.broadcasted_iota(jnp.int32, (tokens, tokens), 1)
        < lax.broadcasted_iota(jnp.int32, (tokens, tokens), 0)
    ).astype(jnp.float32).astype(jnp.bfloat16)

    def settle_shared_sends():
        settle(shared.at[:, 0 : chips - 1, 0], send_sem.at[0])
        settle(seg_all.at[0 : chips - 1, 0], send_sem.at[0])

    lower = level < levels // 2
    outer = jnp.logical_not(inner)
    lower_outer = jnp.logical_and(lower, outer)

    @pl.when(outer)
    def _():
        send_all_owned([far_pairs[-1][0], next_door], [far_pairs[-1][1]])

    @pl.when(jnp.logical_not(lower_outer))
    def _():
        settle_shared_sends()

    @pl.when(jnp.logical_and(lower, inner))
    def _():
        for step in range(1, levels // 2):
            signal(go_sem, chip_at(level - step, row) * 2 + core)

    @pl.when(lower_outer)
    def _():
        pl.semaphore_wait(go_sem, 1)

    @pl.when(outer)
    def _():
        send_all_owned(across_chips, [])

    settle(seg_all.at[0 : chips - 1, 0], seg_recv)
    relays = [remote(
        seg_all.at[:, core], seg_all.at[:, core], send_sem.at[1], relay_recv.at[0], partner
    )]
    settle(owned.at[0, :, 0 : 1 + own_heads], slot_sem)
    settle(shared.at[:, 0 : chips - 1, 0], recv_sem.at[0])
    relays.append(remote(
        shared.at[1:3, :, core], shared.at[1:3, :, core], send_sem.at[1], relay_recv.at[1], partner
    ))
    for copy in loads:
        copy.wait()
    relays[0].wait_recv()
    eye = (
        lax.broadcasted_iota(jnp.int32, (tok, tok), 0)
        == lax.broadcasted_iota(jnp.int32, (tok, tok), 1)
    ).astype(jnp.float32).astype(jnp.bfloat16)
    ids = lax.broadcasted_iota(jnp.int32, (LANES, tok), 0)
    for n in range(devices):
        flipped = (ids == seg_all[n // 2, n % 2]).astype(jnp.float32).astype(jnp.bfloat16)
        hot[n] = lax.dot_general(
            eye, flipped, CONTRACT_LAST, preferred_element_type=jnp.float32
        ).astype(jnp.bfloat16)
    all_hot = hot[...].reshape(tokens, LANES)
    before = jnp.dot(earlier[...], all_hot, preferred_element_type=jnp.float32)
    lane = lax.broadcasted_iota(jnp.int32, (1, LANES), 1)
    limit = jnp.zeros((1, LANES), jnp.int32)
    for r in range(requests):
        limit = jnp.where(lane == r, text_ref[0:1, r : r + 1], limit)
    inside = jnp.where(before < limit.astype(jnp.float32), all_hot.astype(jnp.float32), 0.0)
    text = jnp.dot(
        inside.astype(jnp.bfloat16), jnp.ones((LANES, LANES), jnp.bfloat16),
        preferred_element_type=jnp.float32,
    ) > 0.5
    query_gain, key_gain = query_gain_ref[...], key_gain_ref[...]
    spread = (chips, 2, tok, LANES)
    query_gains[...] = jnp.where(text, query_gain[0:1], query_gain[1:2]).reshape(spread)
    key_gains[...] = jnp.where(text, key_gain[0:1], key_gain[1:2]).reshape(spread)
    same = lax.dot_general(all_hot, all_hot, CONTRACT_LAST, preferred_element_type=jnp.float32)
    bias[...] = jnp.where(same > 0.5, 0.0, MASKED).reshape(chips, 2, tok, tokens)

    scale = 1.0 / math.sqrt(HEAD_DIM)

    def attention_weights(query_n, key_n, query_bias):
        scores = lax.dot_general(
            query_n, key_n, CONTRACT_LAST, preferred_element_type=jnp.float32
        ) * scale + query_bias
        grown = jnp.exp(scores - jnp.max(scores, axis=-1, keepdims=True))
        return (grown * (1.0 / jnp.sum(grown, axis=-1, keepdims=True))).astype(jnp.bfloat16)

    half = (tokens // 2, HEAD_DIM)
    full = (tokens, HEAD_DIM)
    query_n = normed(shared.at[0, :, core][...], query_gains.at[:, core][...]).reshape(half)
    relays[1].wait_recv()
    key_n = normed(shared[1], key_gains[...]).reshape(full)
    part_weights = attention_weights(
        query_n, key_n, bias.at[:, core][...].reshape(tokens // 2, tokens)
    )
    shared_out[...] = jnp.dot(
        part_weights, shared[2].reshape(full), preferred_element_type=jnp.float32
    ).astype(jnp.bfloat16).reshape(chips, tok, HEAD_DIM)

    number = lax.broadcasted_iota(jnp.int32, (LANES, LANES), 0).astype(jnp.float32)
    own_id = jnp.dot(hot[me], number.astype(jnp.bfloat16), preferred_element_type=jnp.float32)
    own_before = jnp.dot(
        earlier[pl.ds(pl.multiple_of(me * tok, tok), tok), :], all_hot,
        preferred_element_type=jnp.float32,
    )
    own_inside = jnp.where(
        own_before < limit.astype(jnp.float32), hot[me].astype(jnp.float32), 0.0
    )
    own_text = jnp.dot(
        own_inside.astype(jnp.bfloat16), jnp.ones((LANES, LANES), jnp.bfloat16),
        preferred_element_type=jnp.float32,
    )
    own_code = 2.0 * own_id + jnp.where(own_text > 0.5, 0.0, 1.0)
    for tile in range(hidden_ref.shape[1] // LANES):
        cols = slice(tile * LANES, (tile + 1) * LANES)
        total = jnp.zeros((tok, LANES), jnp.float32)
        for r in range(requests):
            pair = gate_ref[r, :, cols].astype(jnp.float32)
            for s in range(2):
                total = jnp.where(own_code == float(2 * r + s), pair[s : s + 1], total)
        gate_rows[tile] = total

    far_half = 1 - level // (levels // 2)
    holder = lower_outer
    hold = jnp.logical_and(holder, low)

    def send_shared_result(to_chip):
        remote(
            shared_out.at[to_chip], back.at[chip * per_chip],
            send_sem.at[1], recv_sem.at[1], to_chip * 2 + core,
        )

    def send_owned_result(j, to_chip):
        for a_core in range(2):
            remote(
                owned_out.at[j, to_chip, a_core], back.at[chip * per_chip + own_head(j, core)],
                send_sem.at[1], recv_sem.at[1], to_chip * 2 + a_core,
            )

    for j in range(own_heads):
        settle(owned.at[j, :, 0 : devices - 1], recv_sem.at[2 + j])
        if j == 0:
            @pl.when(jnp.logical_and(holder, core == 1))
            def _():
                signal(done_sem, partner)

            for to_chip in far_chips:
                @pl.when(jnp.logical_not(jnp.logical_and(hold, to_chip // (chips // 2) == far_half)))
                def _():
                    send_shared_result(to_chip)
        flat = (devices, tok, LANES)
        key_n = normed(owned[j, 1], key_gains[...].reshape(flat)).reshape(full)
        value_all = owned[j, 2].reshape(full)
        head = chip * per_chip + own_head(j, core)
        for part in (far_half, 1 - far_half):
            chip_rows = pl.ds(part * (chips // 2), chips // 2)
            rows_in = owned.at[j, 0, pl.ds(part * chips, chips)][...]
            gain_rows = query_gains.at[chip_rows][...].reshape(chips, tok, LANES)
            bias_rows = bias.at[chip_rows][...].reshape(tokens // 2, tokens)
            part_weights = attention_weights(normed(rows_in, gain_rows).reshape(half), key_n, bias_rows)
            owned_out[j, chip_rows] = jnp.dot(
                part_weights, value_all, preferred_element_type=jnp.float32
            ).astype(jnp.bfloat16).reshape(chips // 2, 2, tok, HEAD_DIM)
            for to_chip in far_chips:
                now = to_chip // (chips // 2) == part
                now = jnp.logical_and(now, jnp.logical_not(jnp.logical_and(hold, part == far_half)))

                @pl.when(now)
                def _():
                    send_owned_result(j, to_chip)
        remote(
            owned_out.at[j, chip, 1 - core], back.at[head],
            send_sem.at[1], recv_sem.at[1], partner,
        )

    @pl.when(hold)
    def _():
        pl.semaphore_wait(done_sem, 1)
        for to_chip in far_chips:
            @pl.when(to_chip // (chips // 2) == far_half)
            def _():
                send_shared_result(to_chip)
                for j in range(own_heads):
                    send_owned_result(j, to_chip)

    def finish(head):
        cols = slice(head * HEAD_DIM, (head + 1) * HEAD_DIM)
        out_ref[:, cols] = (
            hidden_ref[:, cols].astype(jnp.float32)
            + gate_rows[head] * back[head].astype(jnp.float32)
        ).astype(jnp.bfloat16)

    @pl.when(lower_outer)
    def _():
        settle_shared_sends()

    settle(seg_all.at[:, core], send_sem.at[1])
    settle(shared.at[1:3, :, core], send_sem.at[1])
    for j in range(own_heads):
        settle(owned.at[j, :, 0 : devices - 1], send_sem.at[1])
    results = back.at[0 : per_chip * (chips - 1) + own_heads]
    settle(results, send_sem.at[1])
    back[chip * per_chip] = shared_out[chip]
    for j in range(own_heads):
        back[chip * per_chip + own_head(j, core)] = owned_out.at[j, chip, core][...]
    settle(results, recv_sem.at[1])
    for head in range(chips * per_chip):
        finish(head)


def fused(
    hidden, queries, key_rows, values, query_gain, key_gain, gate_table, segment, text_count
):
    devices = lax.axis_size("seq")
    chips = devices // 2
    tok, width = hidden.shape
    heads = width // HEAD_DIM
    own_heads = heads // chips // 2
    tokens = devices * tok
    hbm = pl.BlockSpec(memory_space=pl.ANY)
    block = (tok, HEAD_DIM)
    dma = pltpu.SemaphoreType.DMA
    return pl.pallas_call(
        functools.partial(fused_kernel, devices),
        out_shape=jax.ShapeDtypeStruct((tok, width), jnp.bfloat16),
        in_specs=[hbm] * 9,
        out_specs=pl.BlockSpec(memory_space=pltpu.VMEM),
        scratch_shapes=[
            pltpu.VMEM((1, text_count.shape[0]), jnp.int32),
            pltpu.VMEM(hidden.shape, hidden.dtype),
            pltpu.VMEM(query_gain.shape, query_gain.dtype),
            pltpu.VMEM(key_gain.shape, key_gain.dtype),
            pltpu.VMEM(gate_table.shape, gate_table.dtype),
            pltpu.VMEM((3, tok, width), jnp.bfloat16),
            pltpu.VMEM((3, chips, 2) + block, jnp.bfloat16),
            pltpu.VMEM((own_heads, 3, devices) + block, jnp.bfloat16),
            pltpu.VMEM((chips,) + block, jnp.bfloat16),
            pltpu.VMEM((own_heads, chips, 2) + block, jnp.bfloat16),
            pltpu.VMEM((heads,) + block, jnp.bfloat16),
            pltpu.VMEM((chips, 2, 1, tok), jnp.int32),
            pltpu.VMEM((devices, tok, LANES), jnp.bfloat16),
            pltpu.VMEM((tokens, tokens), jnp.bfloat16),
            pltpu.VMEM((chips, 2, tok, LANES), jnp.float32),
            pltpu.VMEM((chips, 2, tok, LANES), jnp.float32),
            pltpu.VMEM((chips, 2, tok, tokens), jnp.float32),
            pltpu.VMEM((heads, tok, LANES), jnp.float32),
            pltpu.SemaphoreType.REGULAR((devices,)),
            pltpu.SemaphoreType.REGULAR,
            pltpu.SemaphoreType.REGULAR,
            dma((5,)),
            dma,
            dma,
            dma,
            dma,
            dma((2,)),
            dma((2 + own_heads,)),
            dma((2,)),
        ],
        compiler_params=pltpu.CompilerParams(
            collective_id=0, has_side_effects=True, vmem_limit_bytes=16 * 1024 * 1024
        ),
    )(*(
        pltpu.with_memory_space_constraint(array, pltpu.HBM)
        for array in (
            segment.reshape(1, tok), queries, key_rows, values,
            text_count.reshape(1, -1), hidden, query_gain, key_gain, gate_table,
        )
    ))


def program(*arrays):
    devices = lax.axis_size("seq")
    tok, width = arrays[0].shape
    requests = arrays[-1].shape[0]
    whole_heads = devices % 8 == 0 and devices > 8 and (width // HEAD_DIM) % (devices // 2) == 0
    odd = whole_heads and width // HEAD_DIM // (devices // 2) % 2 == 1
    if odd and devices * tok <= 512 and requests <= LANES and tok % 16 == 0:
        return fused(*arrays)
    return per_device(*arrays)


def solution(mesh):
    return jax.shard_map(
        program,
        mesh=mesh,
        in_specs=(
            P(("groups", "seq"), None),
            P(("groups", "seq"), None),
            P(("groups", "seq"), None),
            P(("groups", "seq"), None),
            P(),
            P(),
            P("groups", None, None),
            P(("groups", "seq")),
            P("groups"),
        ),
        out_specs=P(("groups", "seq"), None),
        check_vma=False,
    )
```

```python
import functools
import math

import jax
import jax.numpy as jnp
from jax import lax
from jax.experimental import pallas as pl
from jax.experimental.pallas import tpu as pltpu
from jax.sharding import PartitionSpec as P

HEAD_DIM = 128


EPSILON = 1e-06
MASKED = -1e30


def head_norm(rows_in, gains, stream):
    row_count = rows_in.shape[0]
    per_head = rows_in.astype(jnp.float32).reshape(row_count, -1, HEAD_DIM)
    inverse = lax.rsqrt(jnp.mean(per_head * per_head, axis=-1, keepdims=True) + EPSILON)
    gain_rows = jnp.where((stream == 0)[:, None], gains[0][None, :], gains[1][None, :])
    return (per_head * inverse * gain_rows[:, None, :]).astype(jnp.bfloat16).reshape(row_count, -1)


def attend(query_block, block_segment, key_data, value_data, key_segment):
    scores = jnp.einsum(
        "qhd,khd->hqk", query_block, key_data, preferred_element_type=jnp.float32
    ) * (1.0 / math.sqrt(HEAD_DIM))
    allowed = (block_segment[:, None] == key_segment[None, :])[None, :, :]
    scores = jnp.where(allowed, scores, MASKED)
    largest = jnp.max(scores, axis=-1, keepdims=True)
    weights = jnp.exp(scores - largest)
    weights = (weights / jnp.sum(weights, axis=-1, keepdims=True)).astype(jnp.bfloat16)
    return jnp.einsum(
        "hqk,khd->qhd", weights, value_data, preferred_element_type=jnp.float32
    ).astype(jnp.bfloat16)


def per_device(
    hidden, queries, key_rows, values, query_gain, key_gain, gate_table, segment, text_count
):
    tok_rows = hidden.shape[0]
    width_all = hidden.shape[1]
    devices = lax.axis_size("seq")
    requests = text_count.shape[0]
    seg_hot = (segment[:, None] == jnp.arange(requests, dtype=jnp.int32)[None, :]).astype(jnp.int32)
    local_counts = jnp.sum(seg_hot, axis=0)
    all_counts = lax.all_gather(local_counts[None, :], "seq", axis=0, tiled=True)
    lower_rows = (jnp.arange(devices, dtype=jnp.int32) < lax.axis_index("seq")).astype(jnp.int32)
    before = jnp.sum(all_counts * lower_rows[:, None], axis=0)
    position = jnp.sum((jnp.cumsum(seg_hot, axis=0) - seg_hot + before[None, :]) * seg_hot, axis=1)
    text_limit = jnp.sum(seg_hot * text_count[None, :], axis=1)
    stream = (position >= text_limit).astype(jnp.int32)
    query_normed = head_norm(queries, query_gain, stream)
    key_normed = head_norm(key_rows, key_gain, stream)
    groups = 8
    pair_merge = 2
    slices = devices // groups
    cap_rows = 4 * tok_rows // devices + max(1, tok_rows // devices)
    bucket_rows = cap_rows * pair_merge
    head_cols = width_all // groups
    owner_slice = segment // pair_merge
    owner_hot = (owner_slice[:, None] == jnp.arange(slices, dtype=jnp.int32)[None, :]).astype(
        jnp.int32
    )
    owner_rank = jnp.sum((jnp.cumsum(owner_hot, axis=0) - owner_hot) * owner_hot, axis=1)
    slot_place = owner_slice * bucket_rows + owner_rank
    bucket_index = (
        jnp.full((slices * bucket_rows,), tok_rows, jnp.int32)
        .at[slot_place]
        .set(jnp.arange(tok_rows, dtype=jnp.int32))
    )
    stacked = jnp.concatenate(
        [
            query_normed.reshape(tok_rows, groups, head_cols),
            key_normed.reshape(tok_rows, groups, head_cols),
            values.reshape(tok_rows, groups, head_cols),
        ],
        axis=2,
    ).transpose(1, 0, 2)
    outgoing = jnp.take(stacked, bucket_index, axis=1, mode="fill", fill_value=0).reshape(
        devices, bucket_rows, 3 * head_cols
    )
    slot_segment = jnp.take(segment, bucket_index, axis=0, mode="fill", fill_value=-1)
    segment_out = jnp.broadcast_to(slot_segment[None, :], (groups, slices * bucket_rows)).reshape(
        devices, bucket_rows
    )
    arrived, arrived_segment = (
        lax.all_to_all(outgoing, "seq", split_axis=0, concat_axis=0, tiled=True),
        lax.all_to_all(segment_out, "seq", split_axis=0, concat_axis=0, tiled=True),
    )
    slot_count = devices * bucket_rows
    per_head = head_cols // HEAD_DIM
    slot_data = arrived.reshape(slot_count, 3 * head_cols)
    query_all = slot_data[:, :head_cols].reshape(slot_count, per_head, HEAD_DIM)
    key_all = slot_data[:, head_cols : 2 * head_cols].reshape(slot_count, per_head, HEAD_DIM)
    value_all = slot_data[:, 2 * head_cols :].reshape(slot_count, per_head, HEAD_DIM)
    key_segment = arrived_segment.reshape(slot_count)
    if slot_count % 512 == 0:
        block_rows = 512
    elif slot_count % 256 == 0:
        block_rows = 256
    else:
        block_rows = slot_count

    def one_block(first_row):
        return attend(query_all, key_segment, key_all, value_all, key_segment)

    results = lax.map(one_block, jnp.arange(slot_count // block_rows, dtype=jnp.int32) * block_rows)
    returning = results.reshape(devices, bucket_rows, head_cols)
    returned = lax.all_to_all(returning, "seq", split_axis=0, concat_axis=0, tiled=True)
    returned = returned.reshape(groups, slices * bucket_rows, head_cols)
    attention = (
        jnp.take(returned, slot_place, axis=1).transpose(1, 0, 2).reshape(tok_rows, width_all)
    )
    gate_rows = jnp.take(gate_table.reshape(requests * 2, width_all), segment * 2 + stream, axis=0)
    mixed = hidden.astype(jnp.float32) + gate_rows.astype(jnp.float32) * attention.astype(
        jnp.float32
    )
    return mixed.astype(jnp.bfloat16)


LANES = 128
CONTRACT_LAST = (((1,), (1,)), ((), ()))


def normed(rows, gain_rows):
    wide = rows.astype(jnp.float32)
    inverse = lax.rsqrt(jnp.mean(wide * wide, axis=-1, keepdims=True) + EPSILON)
    return (wide * inverse * gain_rows).astype(jnp.bfloat16)


def fused_kernel(
    devices, segment_hbm, query_hbm, key_hbm, value_hbm,
    text_hbm, hidden_hbm, query_gain_hbm, key_gain_hbm, gate_hbm, out_ref,
    text_ref, hidden_ref, query_gain_ref, key_gain_ref, gate_ref,
    staged, shared, owned, passing, shared_out, owned_out, back, seg_all, hot, earlier,
    query_gains, key_gains, bias, gate_rows,
    here_sem, go_sem, done_sem, load_sem, seg_own_sem, stage_sem, slot_sem,
    seg_recv, send_sem, recv_sem, relay_recv,
):
    chips = devices // 2
    levels = chips // 2
    tok = hidden_hbm.shape[0]
    per_chip = hidden_hbm.shape[1] // HEAD_DIM // chips
    own_heads = per_chip // 2
    requests = gate_hbm.shape[0]
    tokens = devices * tok
    me = lax.axis_index("seq")
    chip, core = me // 2, me % 2
    row, level = chip % 2, chip // 2
    partner = me + 1 - 2 * core
    sources = (query_hbm, key_hbm, value_hbm)

    def columns(head):
        return pl.ds(pl.multiple_of(head * HEAD_DIM, HEAD_DIM), HEAD_DIM)

    def chip_at(a_level, a_row):
        return a_level * 2 + a_row

    def signal(semaphore, device):
        pl.semaphore_signal(
            semaphore, inc=1, device_id={"seq": device}, device_id_type=pl.DeviceIdType.MESH
        )

    def remote(src, dst, send, recv, device):
        copy = pltpu.make_async_remote_copy(
            src_ref=src, dst_ref=dst, send_sem=send, recv_sem=recv,
            device_id={"seq": device}, device_id_type=pl.DeviceIdType.MESH,
        )
        copy.start()
        return copy

    def settle(ref, semaphore):
        pltpu.make_async_copy(ref, ref, semaphore).wait()

    toward = 1 - 2 * (level // (levels // 2))
    near_first = [(level + levels + toward * step) % levels for step in range(1, levels)]
    far_first = [(level + levels - toward * step) % levels for step in range(1, levels)]
    orders = []
    for start in range(levels):
        first = start + (1 if start < levels // 2 else -1)
        rest = list(range(start - 1, -1, -1)) + list(range(start + 1, levels))
        orders.append([first] + [n for n in rest if n != first])

    def pick(values):
        result = values[0]
        for start in range(1, levels):
            result = jnp.where(level == start, values[start], result)
        return result

    met = [pick([order[place] for order in orders]) for place in range(levels - 1)]
    near_chips = []
    for place, a_level in enumerate(near_first):
        near_chips.append(chip_at(a_level, row))
        near_chips.append(chip_at(a_level, 1 - row))
    near_chips.append(chip_at(level, 1 - row))
    for part, source in enumerate(sources):
        pltpu.make_async_copy(source, staged.at[part], stage_sem).start()

    barrier = pltpu.get_barrier_semaphore()

    @pl.when(me > 0)
    def _():
        pl.semaphore_wait(barrier, (level + levels - 1) // levels + row + core)

    @pl.when(level + 1 < levels)
    def _():
        signal(barrier, me + 4)

    @pl.when(row == 0)
    def _():
        signal(barrier, me + 2)

    @pl.when(core == 0)
    def _():
        signal(barrier, me + 1)

    for down in range(levels):
        for row_down in range(2):
            for core_down in range(2):
                if down + row_down + core_down > 0:
                    fits = level >= down
                    if row_down:
                        fits = jnp.logical_and(fits, row == 1)
                    if core_down:
                        fits = jnp.logical_and(fits, core == 1)

                    @pl.when(fits)
                    def _():
                        signal(here_sem.at[me], me - 4 * down - 2 * row_down - core_down)

    def vouched(condition, a_level, a_row, a_core):
        @pl.when(condition)
        def _():
            pl.semaphore_wait(here_sem.at[chip_at(a_level, a_row) * 2 + a_core], 1)

    seg_own = pltpu.make_async_copy(segment_hbm, seg_all.at[chip, core], seg_own_sem)
    seg_own.start()
    for part, source in enumerate(sources):
        pltpu.make_async_copy(
            source.at[:, columns(chip * per_chip)], shared.at[part, chip, core], slot_sem
        ).start()
        for j in range(own_heads):
            pltpu.make_async_copy(
                source.at[:, columns(chip * per_chip + 1 + core * own_heads + j)],
                owned.at[j, part, me], slot_sem,
            ).start()
    loads = [
        pltpu.make_async_copy(source, target, load_sem.at[place])
        for place, (source, target) in enumerate(
            (
                (text_hbm, text_ref), (query_gain_hbm, query_gain_ref),
                (key_gain_hbm, key_gain_ref), (gate_hbm, gate_ref), (hidden_hbm, hidden_ref),
            )
        )
    ]
    for copy in loads:
        copy.start()
    settle(staged, stage_sem)
    seg_own.wait()

    def own_head(j, a_core):
        return 1 + a_core * own_heads + j

    def send_owned(to_chip, a_core):
        for j in range(own_heads):
            remote(
                staged.at[:, :, columns(to_chip * per_chip + own_head(j, a_core))],
                owned.at[j, :, me], send_sem.at[1], recv_sem.at[2 + j], to_chip * 2 + a_core,
            )

    def send_shared(to_chip):
        device = to_chip * 2 + core
        own_ids = seg_all.at[chip, core]
        remote(own_ids, own_ids, send_sem.at[0], seg_recv, device)
        remote(
            staged.at[:, :, columns(to_chip * per_chip)], shared.at[:, chip, core],
            send_sem.at[0], recv_sem.at[0], device,
        )

    low = core == 0
    upper = row == 0
    low_upper = jnp.logical_and(low, upper)

    for place, a_level in enumerate(met):
        above = a_level > level
        vouched(above, a_level, row, core)
        send_shared(chip_at(a_level, row))
        if place == 0:
            @pl.when(low)
            def _():
                send_owned(chip_at(met[0], row), 0)

            vouched(low, level, row, 1)
            vouched(jnp.logical_and(low, above), a_level, row, 1)

            @pl.when(jnp.logical_not(low))
            def _():
                send_owned(chip_at(met[0], row), 0)

            continue
        if place == 1:
            vouched(upper, level, 1, core)
            send_shared(chip_at(level, 1 - row))
            vouched(jnp.logical_and(met[0] > level, upper), met[0], 1, core)
            send_shared(chip_at(met[0], 1 - row))
        vouched(jnp.logical_and(above, upper), a_level, 1, core)
        send_shared(chip_at(a_level, 1 - row))

    send_owned(chip, 1 - core)
    vouched(low_upper, level, 1, 1)
    vouched(jnp.logical_and(low_upper, met[0] > level), met[0], 1, 1)
    for a_level in met[1:]:
        vouched(jnp.logical_and(low, a_level > level), a_level, row, 1)
        vouched(jnp.logical_and(low_upper, a_level > level), a_level, 1, 1)

    far_pairs = [(chip_at(a_level, 1 - row), chip_at(a_level, row)) for a_level in far_first]
    next_door = chip_at(level, 1 - row)
    across_chips = [to_chip for pair in far_pairs[:-1] for to_chip in pair]

    def send_all_owned(to_chips, last_chips, but=None):
        for to_chip in to_chips:
            send_owned(to_chip, 0)
        for to_chip in to_chips + last_chips:
            if to_chip is but:
                @pl.when(jnp.logical_not(shifts))
                def _():
                    send_owned(to_chip, 1)
            else:
                send_owned(to_chip, 1)

    inner = jnp.logical_or(level == levels // 2 - 1, level == levels // 2)

    @pl.when(inner)
    def _():
        send_all_owned(across_chips + [far_pairs[-1][0], next_door], [far_pairs[-1][1]])

    earlier[...] = (
        lax.broadcasted_iota(jnp.int32, (tokens, tokens), 1)
        < lax.broadcasted_iota(jnp.int32, (tokens, tokens), 0)
    ).astype(jnp.float32).astype(jnp.bfloat16)

    def settle_shared_sends():
        settle(shared.at[:, 0 : chips - 1, 0], send_sem.at[0])
        settle(seg_all.at[0 : chips - 1, 0], send_sem.at[0])

    lower = level < levels // 2
    shifts = jnp.logical_and(lower, row == 1)
    shifted_chip = chip_at(levels // 2, 0)
    outer = jnp.logical_not(inner)
    lower_outer = jnp.logical_and(lower, outer)

    @pl.when(outer)
    def _():
        send_all_owned([far_pairs[-1][0], next_door], [far_pairs[-1][1]])

    @pl.when(jnp.logical_not(lower_outer))
    def _():
        settle_shared_sends()

    @pl.when(jnp.logical_and(lower, inner))
    def _():
        for step in range(1, levels // 2):
            signal(go_sem, chip_at(level - step, row) * 2 + core)

    passes = jnp.logical_and(lower_outer, row == 0)

    @pl.when(jnp.logical_and(lower_outer, row == 1))
    def _():
        for j in range(own_heads):
            remote(
                staged.at[:, :, columns(shifted_chip * per_chip + own_head(j, 1))],
                passing.at[j], send_sem.at[1], relay_recv.at[2], me - 2,
            )

    @pl.when(lower_outer)
    def _():
        pl.semaphore_wait(go_sem, 1)

    @pl.when(outer)
    def _():
        send_all_owned(across_chips, [], across_chips[2])

    @pl.when(passes)
    def _():
        settle(passing, relay_recv.at[2])
        for j in range(own_heads):
            remote(
                passing.at[j], owned.at[j, :, me + 2],
                send_sem.at[1], recv_sem.at[2 + j], shifted_chip * 2 + 1,
            )

    settle(seg_all.at[0 : chips - 1, 0], seg_recv)
    relays = [remote(
        seg_all.at[:, core], seg_all.at[:, core], send_sem.at[1], relay_recv.at[0], partner
    )]
    settle(owned.at[0, :, 0 : 1 + own_heads], slot_sem)
    settle(shared.at[:, 0 : chips - 1, 0], recv_sem.at[0])
    relays.append(remote(
        shared.at[1:3, :, core], shared.at[1:3, :, core], send_sem.at[1], relay_recv.at[1], partner
    ))
    for copy in loads:
        copy.wait()
    relays[0].wait_recv()
    eye = (
        lax.broadcasted_iota(jnp.int32, (tok, tok), 0)
        == lax.broadcasted_iota(jnp.int32, (tok, tok), 1)
    ).astype(jnp.float32).astype(jnp.bfloat16)
    ids = lax.broadcasted_iota(jnp.int32, (LANES, tok), 0)
    for n in range(devices):
        flipped = (ids == seg_all[n // 2, n % 2]).astype(jnp.float32).astype(jnp.bfloat16)
        hot[n] = lax.dot_general(
            eye, flipped, CONTRACT_LAST, preferred_element_type=jnp.float32
        ).astype(jnp.bfloat16)
    all_hot = hot[...].reshape(tokens, LANES)
    before = jnp.dot(earlier[...], all_hot, preferred_element_type=jnp.float32)
    lane = lax.broadcasted_iota(jnp.int32, (1, LANES), 1)
    limit = jnp.zeros((1, LANES), jnp.int32)
    for r in range(requests):
        limit = jnp.where(lane == r, text_ref[0:1, r : r + 1], limit)
    inside = jnp.where(before < limit.astype(jnp.float32), all_hot.astype(jnp.float32), 0.0)
    text = jnp.dot(
        inside.astype(jnp.bfloat16), jnp.ones((LANES, LANES), jnp.bfloat16),
        preferred_element_type=jnp.float32,
    ) > 0.5
    query_gain, key_gain = query_gain_ref[...], key_gain_ref[...]
    spread = (chips, 2, tok, LANES)
    query_gains[...] = jnp.where(text, query_gain[0:1], query_gain[1:2]).reshape(spread)
    key_gains[...] = jnp.where(text, key_gain[0:1], key_gain[1:2]).reshape(spread)
    same = lax.dot_general(all_hot, all_hot, CONTRACT_LAST, preferred_element_type=jnp.float32)
    bias[...] = jnp.where(same > 0.5, 0.0, MASKED).reshape(chips, 2, tok, tokens)

    scale = 1.0 / math.sqrt(HEAD_DIM)

    def attention_weights(query_n, key_n, query_bias):
        scores = lax.dot_general(
            query_n, key_n, CONTRACT_LAST, preferred_element_type=jnp.float32
        ) * scale + query_bias
        grown = jnp.exp(scores - jnp.max(scores, axis=-1, keepdims=True))
        return (grown * (1.0 / jnp.sum(grown, axis=-1, keepdims=True))).astype(jnp.bfloat16)

    half = (tokens // 2, HEAD_DIM)
    full = (tokens, HEAD_DIM)
    query_n = normed(shared.at[0, :, core][...], query_gains.at[:, core][...]).reshape(half)
    relays[1].wait_recv()
    key_n = normed(shared[1], key_gains[...]).reshape(full)
    part_weights = attention_weights(
        query_n, key_n, bias.at[:, core][...].reshape(tokens // 2, tokens)
    )
    shared_out[...] = jnp.dot(
        part_weights, shared[2].reshape(full), preferred_element_type=jnp.float32
    ).astype(jnp.bfloat16).reshape(chips, tok, HEAD_DIM)

    number = lax.broadcasted_iota(jnp.int32, (LANES, LANES), 0).astype(jnp.float32)
    own_id = jnp.dot(hot[me], number.astype(jnp.bfloat16), preferred_element_type=jnp.float32)
    own_before = jnp.dot(
        earlier[pl.ds(pl.multiple_of(me * tok, tok), tok), :], all_hot,
        preferred_element_type=jnp.float32,
    )
    own_inside = jnp.where(
        own_before < limit.astype(jnp.float32), hot[me].astype(jnp.float32), 0.0
    )
    own_text = jnp.dot(
        own_inside.astype(jnp.bfloat16), jnp.ones((LANES, LANES), jnp.bfloat16),
        preferred_element_type=jnp.float32,
    )
    own_code = 2.0 * own_id + jnp.where(own_text > 0.5, 0.0, 1.0)
    for tile in range(hidden_ref.shape[1] // LANES):
        cols = slice(tile * LANES, (tile + 1) * LANES)
        total = jnp.zeros((tok, LANES), jnp.float32)
        for r in range(requests):
            pair = gate_ref[r, :, cols].astype(jnp.float32)
            for s in range(2):
                total = jnp.where(own_code == float(2 * r + s), pair[s : s + 1], total)
        gate_rows[tile] = total

    holder = lower_outer
    hold = jnp.logical_and(holder, low)
    lower_half = level < levels // 2
    lower_chips = list(range(chips // 2))
    upper_chips = list(range(chips // 2, chips))

    def send_shared_result(to_chip):
        remote(
            shared_out.at[to_chip], back.at[chip * per_chip],
            send_sem.at[1], recv_sem.at[1], to_chip * 2 + core,
        )

    def send_owned_result(j, to_chip):
        for a_core in range(2):
            remote(
                owned_out.at[j, to_chip, a_core], back.at[chip * per_chip + own_head(j, core)],
                send_sem.at[1], recv_sem.at[1], to_chip * 2 + a_core,
            )

    def send_results(to_chips, condition, send):
        for to_chip in to_chips:
            @pl.when(jnp.logical_and(condition, chip != to_chip))
            def _():
                send(to_chip)

    def send_shared_results(to_chips, condition):
        send_results(to_chips, condition, send_shared_result)

    def send_owned_results(j, to_chips, condition):
        send_results(to_chips, condition, functools.partial(send_owned_result, j))

    for j in range(own_heads):
        settle(owned.at[j, :, 0 : devices - 1], recv_sem.at[2 + j])
        if j == 0:
            @pl.when(jnp.logical_and(holder, core == 1))
            def _():
                signal(done_sem, partner)

            send_shared_results(lower_chips[2:], lower_half)
            send_shared_results(lower_chips[:2], chip >= 0)
            send_shared_results(upper_chips, jnp.logical_not(hold))
        flat = (devices, tok, LANES)
        key_n = normed(owned[j, 1], key_gains[...].reshape(flat)).reshape(full)
        value_all = owned[j, 2].reshape(full)
        head = chip * per_chip + own_head(j, core)
        for place, to_chips in enumerate((lower_chips, upper_chips)):
            chip_rows = pl.ds(place * (chips // 2), chips // 2)
            rows_in = owned[j, 0, place * chips : (place + 1) * chips]
            gain_rows = query_gains[chip_rows].reshape(chips, tok, LANES)
            query_n = normed(rows_in, gain_rows).reshape(half)
            bias_rows = bias[chip_rows].reshape(tokens // 2, tokens)
            owned_out[j, chip_rows] = jnp.dot(
                attention_weights(query_n, key_n, bias_rows), value_all,
                preferred_element_type=jnp.float32,
            ).astype(jnp.bfloat16).reshape(chips // 2, 2, tok, HEAD_DIM)
            if place == 0:
                send_owned_results(j, lower_chips[:2], chip >= 0)
                send_owned_results(j, lower_chips[2:], lower_half)
        send_owned_results(j, lower_chips[2:], jnp.logical_not(lower_half))
        send_owned_results(j, upper_chips, jnp.logical_not(hold))
        if j == 0:
            send_shared_results(lower_chips[2:], jnp.logical_not(lower_half))
        remote(
            owned_out.at[j, chip, 1 - core], back.at[head],
            send_sem.at[1], recv_sem.at[1], partner,
        )

    @pl.when(hold)
    def _():
        pl.semaphore_wait(done_sem, 1)
        for to_chip in upper_chips:
            send_shared_result(to_chip)
            for j in range(own_heads):
                send_owned_result(j, to_chip)

    def finish(head):
        cols = slice(head * HEAD_DIM, (head + 1) * HEAD_DIM)
        out_ref[:, cols] = (
            hidden_ref[:, cols].astype(jnp.float32)
            + gate_rows[head] * back[head].astype(jnp.float32)
        ).astype(jnp.bfloat16)

    @pl.when(lower_outer)
    def _():
        settle_shared_sends()

    @pl.when(passes)
    def _():
        settle(passing, send_sem.at[1])

    settle(seg_all.at[:, core], send_sem.at[1])
    settle(shared.at[1:3, :, core], send_sem.at[1])
    for j in range(own_heads):
        settle(owned.at[j, :, 0 : devices - 1], send_sem.at[1])
    results = back.at[0 : per_chip * (chips - 1) + own_heads]
    settle(results, send_sem.at[1])
    back[chip * per_chip] = shared_out[chip]
    for j in range(own_heads):
        back[chip * per_chip + own_head(j, core)] = owned_out.at[j, chip, core][...]
    settle(results, recv_sem.at[1])
    for head in range(chips * per_chip):
        finish(head)


def fused(
    hidden, queries, key_rows, values, query_gain, key_gain, gate_table, segment, text_count
):
    devices = lax.axis_size("seq")
    chips = devices // 2
    tok, width = hidden.shape
    heads = width // HEAD_DIM
    own_heads = heads // chips // 2
    tokens = devices * tok
    hbm = pl.BlockSpec(memory_space=pl.ANY)
    block = (tok, HEAD_DIM)
    dma = pltpu.SemaphoreType.DMA
    return pl.pallas_call(
        functools.partial(fused_kernel, devices),
        out_shape=jax.ShapeDtypeStruct((tok, width), jnp.bfloat16),
        in_specs=[hbm] * 9,
        out_specs=pl.BlockSpec(memory_space=pltpu.VMEM),
        scratch_shapes=[
            pltpu.VMEM((1, text_count.shape[0]), jnp.int32),
            pltpu.VMEM(hidden.shape, hidden.dtype),
            pltpu.VMEM(query_gain.shape, query_gain.dtype),
            pltpu.VMEM(key_gain.shape, key_gain.dtype),
            pltpu.VMEM(gate_table.shape, gate_table.dtype),
            pltpu.VMEM((3, tok, width), jnp.bfloat16),
            pltpu.VMEM((3, chips, 2) + block, jnp.bfloat16),
            pltpu.VMEM((own_heads, 3, devices) + block, jnp.bfloat16),
            pltpu.VMEM((own_heads, 3) + block, jnp.bfloat16),
            pltpu.VMEM((chips,) + block, jnp.bfloat16),
            pltpu.VMEM((own_heads, chips, 2) + block, jnp.bfloat16),
            pltpu.VMEM((heads,) + block, jnp.bfloat16),
            pltpu.VMEM((chips, 2, 1, tok), jnp.int32),
            pltpu.VMEM((devices, tok, LANES), jnp.bfloat16),
            pltpu.VMEM((tokens, tokens), jnp.bfloat16),
            pltpu.VMEM((chips, 2, tok, LANES), jnp.float32),
            pltpu.VMEM((chips, 2, tok, LANES), jnp.float32),
            pltpu.VMEM((chips, 2, tok, tokens), jnp.float32),
            pltpu.VMEM((heads, tok, LANES), jnp.float32),
            pltpu.SemaphoreType.REGULAR((devices,)),
            pltpu.SemaphoreType.REGULAR,
            pltpu.SemaphoreType.REGULAR,
            dma((5,)),
            dma,
            dma,
            dma,
            dma,
            dma((2,)),
            dma((2 + own_heads,)),
            dma((3,)),
        ],
        compiler_params=pltpu.CompilerParams(
            collective_id=0, has_side_effects=True, vmem_limit_bytes=16 * 1024 * 1024
        ),
    )(*(
        pltpu.with_memory_space_constraint(array, pltpu.HBM)
        for array in (
            segment.reshape(1, tok), queries, key_rows, values,
            text_count.reshape(1, -1), hidden, query_gain, key_gain, gate_table,
        )
    ))


def program(*arrays):
    devices = lax.axis_size("seq")
    tok, width = arrays[0].shape
    requests = arrays[-1].shape[0]
    whole_heads = devices % 8 == 0 and devices > 8 and (width // HEAD_DIM) % (devices // 2) == 0
    odd = whole_heads and width // HEAD_DIM // (devices // 2) % 2 == 1
    if odd and devices * tok <= 512 and requests <= LANES and tok % 16 == 0:
        return fused(*arrays)
    return per_device(*arrays)


def solution(mesh):
    return jax.shard_map(
        program,
        mesh=mesh,
        in_specs=(
            P(("groups", "seq"), None),
            P(("groups", "seq"), None),
            P(("groups", "seq"), None),
            P(("groups", "seq"), None),
            P(),
            P(),
            P("groups", None, None),
            P(("groups", "seq")),
            P("groups"),
        ),
        out_specs=P(("groups", "seq"), None),
        check_vma=False,
    )
```

```python
import functools
import math

import jax
import jax.numpy as jnp
from jax import lax
from jax.experimental import pallas as pl
from jax.experimental.pallas import tpu as pltpu
from jax.sharding import PartitionSpec as P

HEAD_DIM = 128


EPSILON = 1e-06
MASKED = -1e30


def head_norm(rows_in, gains, stream):
    row_count = rows_in.shape[0]
    per_head = rows_in.astype(jnp.float32).reshape(row_count, -1, HEAD_DIM)
    inverse = lax.rsqrt(jnp.mean(per_head * per_head, axis=-1, keepdims=True) + EPSILON)
    gain_rows = jnp.where((stream == 0)[:, None], gains[0][None, :], gains[1][None, :])
    return (per_head * inverse * gain_rows[:, None, :]).astype(jnp.bfloat16).reshape(row_count, -1)


def attend(query_block, block_segment, key_data, value_data, key_segment):
    scores = jnp.einsum(
        "qhd,khd->hqk", query_block, key_data, preferred_element_type=jnp.float32
    ) * (1.0 / math.sqrt(HEAD_DIM))
    allowed = (block_segment[:, None] == key_segment[None, :])[None, :, :]
    scores = jnp.where(allowed, scores, MASKED)
    largest = jnp.max(scores, axis=-1, keepdims=True)
    weights = jnp.exp(scores - largest)
    weights = (weights / jnp.sum(weights, axis=-1, keepdims=True)).astype(jnp.bfloat16)
    return jnp.einsum(
        "hqk,khd->qhd", weights, value_data, preferred_element_type=jnp.float32
    ).astype(jnp.bfloat16)


def per_device(
    hidden, queries, key_rows, values, query_gain, key_gain, gate_table, segment, text_count
):
    tok_rows = hidden.shape[0]
    width_all = hidden.shape[1]
    devices = lax.axis_size("seq")
    requests = text_count.shape[0]
    seg_hot = (segment[:, None] == jnp.arange(requests, dtype=jnp.int32)[None, :]).astype(jnp.int32)
    local_counts = jnp.sum(seg_hot, axis=0)
    all_counts = lax.all_gather(local_counts[None, :], "seq", axis=0, tiled=True)
    lower_rows = (jnp.arange(devices, dtype=jnp.int32) < lax.axis_index("seq")).astype(jnp.int32)
    before = jnp.sum(all_counts * lower_rows[:, None], axis=0)
    position = jnp.sum((jnp.cumsum(seg_hot, axis=0) - seg_hot + before[None, :]) * seg_hot, axis=1)
    text_limit = jnp.sum(seg_hot * text_count[None, :], axis=1)
    stream = (position >= text_limit).astype(jnp.int32)
    query_normed = head_norm(queries, query_gain, stream)
    key_normed = head_norm(key_rows, key_gain, stream)
    groups = 8
    pair_merge = 2
    slices = devices // groups
    cap_rows = 4 * tok_rows // devices + max(1, tok_rows // devices)
    bucket_rows = cap_rows * pair_merge
    head_cols = width_all // groups
    owner_slice = segment // pair_merge
    owner_hot = (owner_slice[:, None] == jnp.arange(slices, dtype=jnp.int32)[None, :]).astype(
        jnp.int32
    )
    owner_rank = jnp.sum((jnp.cumsum(owner_hot, axis=0) - owner_hot) * owner_hot, axis=1)
    slot_place = owner_slice * bucket_rows + owner_rank
    bucket_index = (
        jnp.full((slices * bucket_rows,), tok_rows, jnp.int32)
        .at[slot_place]
        .set(jnp.arange(tok_rows, dtype=jnp.int32))
    )
    stacked = jnp.concatenate(
        [
            query_normed.reshape(tok_rows, groups, head_cols),
            key_normed.reshape(tok_rows, groups, head_cols),
            values.reshape(tok_rows, groups, head_cols),
        ],
        axis=2,
    ).transpose(1, 0, 2)
    outgoing = jnp.take(stacked, bucket_index, axis=1, mode="fill", fill_value=0).reshape(
        devices, bucket_rows, 3 * head_cols
    )
    slot_segment = jnp.take(segment, bucket_index, axis=0, mode="fill", fill_value=-1)
    segment_out = jnp.broadcast_to(slot_segment[None, :], (groups, slices * bucket_rows)).reshape(
        devices, bucket_rows
    )
    arrived, arrived_segment = (
        lax.all_to_all(outgoing, "seq", split_axis=0, concat_axis=0, tiled=True),
        lax.all_to_all(segment_out, "seq", split_axis=0, concat_axis=0, tiled=True),
    )
    slot_count = devices * bucket_rows
    per_head = head_cols // HEAD_DIM
    slot_data = arrived.reshape(slot_count, 3 * head_cols)
    query_all = slot_data[:, :head_cols].reshape(slot_count, per_head, HEAD_DIM)
    key_all = slot_data[:, head_cols : 2 * head_cols].reshape(slot_count, per_head, HEAD_DIM)
    value_all = slot_data[:, 2 * head_cols :].reshape(slot_count, per_head, HEAD_DIM)
    key_segment = arrived_segment.reshape(slot_count)
    if slot_count % 512 == 0:
        block_rows = 512
    elif slot_count % 256 == 0:
        block_rows = 256
    else:
        block_rows = slot_count

    def one_block(first_row):
        return attend(query_all, key_segment, key_all, value_all, key_segment)

    results = lax.map(one_block, jnp.arange(slot_count // block_rows, dtype=jnp.int32) * block_rows)
    returning = results.reshape(devices, bucket_rows, head_cols)
    returned = lax.all_to_all(returning, "seq", split_axis=0, concat_axis=0, tiled=True)
    returned = returned.reshape(groups, slices * bucket_rows, head_cols)
    attention = (
        jnp.take(returned, slot_place, axis=1).transpose(1, 0, 2).reshape(tok_rows, width_all)
    )
    gate_rows = jnp.take(gate_table.reshape(requests * 2, width_all), segment * 2 + stream, axis=0)
    mixed = hidden.astype(jnp.float32) + gate_rows.astype(jnp.float32) * attention.astype(
        jnp.float32
    )
    return mixed.astype(jnp.bfloat16)


LANES = 128
CONTRACT_LAST = (((1,), (1,)), ((), ()))


def normed(rows, gain_rows):
    wide = rows.astype(jnp.float32)
    inverse = lax.rsqrt(jnp.mean(wide * wide, axis=-1, keepdims=True) + EPSILON)
    return (wide * inverse * gain_rows).astype(jnp.bfloat16)


def fused_kernel(
    devices, segment_hbm, query_hbm, key_hbm, value_hbm,
    text_hbm, hidden_hbm, query_gain_hbm, key_gain_hbm, gate_hbm, out_ref,
    text_ref, hidden_ref, query_gain_ref, key_gain_ref, gate_ref,
    staged, shared, owned, passing, shared_out, owned_out, back, seg_all, hot, earlier,
    query_gains, key_gains, bias, gate_rows,
    here_sem, go_sem, done_sem, load_sem, seg_own_sem, stage_sem, slot_sem,
    seg_recv, send_sem, recv_sem, relay_recv,
):
    chips = devices // 2
    levels = chips // 2
    tok = hidden_hbm.shape[0]
    per_chip = hidden_hbm.shape[1] // HEAD_DIM // chips
    own_heads = per_chip // 2
    requests = gate_hbm.shape[0]
    tokens = devices * tok
    me = lax.axis_index("seq")
    chip, core = me // 2, me % 2
    row, level = chip % 2, chip // 2
    partner = me + 1 - 2 * core
    sources = (query_hbm, key_hbm, value_hbm)

    def columns(head):
        return pl.ds(pl.multiple_of(head * HEAD_DIM, HEAD_DIM), HEAD_DIM)

    def chip_at(a_level, a_row):
        return a_level * 2 + a_row

    def signal(semaphore, device):
        pl.semaphore_signal(
            semaphore, inc=1, device_id={"seq": device}, device_id_type=pl.DeviceIdType.MESH
        )

    def remote(src, dst, send, recv, device):
        copy = pltpu.make_async_remote_copy(
            src_ref=src, dst_ref=dst, send_sem=send, recv_sem=recv,
            device_id={"seq": device}, device_id_type=pl.DeviceIdType.MESH,
        )
        copy.start()
        return copy

    def settle(ref, semaphore):
        pltpu.make_async_copy(ref, ref, semaphore).wait()

    toward = 1 - 2 * (level // (levels // 2))
    near_first = [(level + levels + toward * step) % levels for step in range(1, levels)]
    far_first = [(level + levels - toward * step) % levels for step in range(1, levels)]
    orders = []
    for start in range(levels):
        first = start + (1 if start < levels // 2 else -1)
        rest = list(range(start - 1, -1, -1)) + list(range(start + 1, levels))
        orders.append([first] + [n for n in rest if n != first])

    def pick(values):
        result = values[0]
        for start in range(1, levels):
            result = jnp.where(level == start, values[start], result)
        return result

    met = [pick([order[place] for order in orders]) for place in range(levels - 1)]
    near_chips = []
    for place, a_level in enumerate(near_first):
        near_chips.append(chip_at(a_level, row))
        near_chips.append(chip_at(a_level, 1 - row))
    near_chips.append(chip_at(level, 1 - row))
    for part, source in enumerate(sources):
        pltpu.make_async_copy(source, staged.at[part], stage_sem).start()

    barrier = pltpu.get_barrier_semaphore()

    @pl.when(me > 0)
    def _():
        pl.semaphore_wait(barrier, (level + levels - 1) // levels + row + core)

    @pl.when(level + 1 < levels)
    def _():
        signal(barrier, me + 4)

    @pl.when(row == 0)
    def _():
        signal(barrier, me + 2)

    @pl.when(core == 0)
    def _():
        signal(barrier, me + 1)

    for down in range(levels):
        for row_down in range(2):
            for core_down in range(2):
                if down + row_down + core_down > 0:
                    fits = level >= down
                    if row_down:
                        fits = jnp.logical_and(fits, row == 1)
                    if core_down:
                        fits = jnp.logical_and(fits, core == 1)

                    @pl.when(fits)
                    def _():
                        signal(here_sem.at[me], me - 4 * down - 2 * row_down - core_down)

    def vouched(condition, a_level, a_row, a_core):
        @pl.when(condition)
        def _():
            pl.semaphore_wait(here_sem.at[chip_at(a_level, a_row) * 2 + a_core], 1)

    seg_own = pltpu.make_async_copy(segment_hbm, seg_all.at[chip, core], seg_own_sem)
    seg_own.start()
    for part, source in enumerate(sources):
        pltpu.make_async_copy(
            source.at[:, columns(chip * per_chip)], shared.at[part, chip, core], slot_sem
        ).start()
        for j in range(own_heads):
            pltpu.make_async_copy(
                source.at[:, columns(chip * per_chip + 1 + core * own_heads + j)],
                owned.at[j, part, me], slot_sem,
            ).start()
    loads = [
        pltpu.make_async_copy(source, target, load_sem)
        for source, target in (
            (text_hbm, text_ref), (query_gain_hbm, query_gain_ref),
            (key_gain_hbm, key_gain_ref), (gate_hbm, gate_ref), (hidden_hbm, hidden_ref),
        )
    ]
    for copy in loads:
        copy.start()
    settle(staged, stage_sem)
    seg_own.wait()

    def own_head(j, a_core):
        return 1 + a_core * own_heads + j

    def send_owned(to_chip, a_core):
        for j in range(own_heads):
            remote(
                staged.at[:, :, columns(to_chip * per_chip + own_head(j, a_core))],
                owned.at[j, :, me], send_sem.at[1], recv_sem.at[2 + j], to_chip * 2 + a_core,
            )

    def send_shared(to_chip):
        device = to_chip * 2 + core
        own_ids = seg_all.at[chip, core]
        remote(own_ids, own_ids, send_sem.at[0], seg_recv, device)
        remote(
            staged.at[:, :, columns(to_chip * per_chip)], shared.at[:, chip, core],
            send_sem.at[0], recv_sem.at[0], device,
        )

    low = core == 0
    upper = row == 0
    low_upper = jnp.logical_and(low, upper)

    for place, a_level in enumerate(met):
        above = a_level > level
        vouched(above, a_level, row, core)
        send_shared(chip_at(a_level, row))
        if place == 0:
            @pl.when(low)
            def _():
                send_owned(chip_at(met[0], row), 0)

            vouched(low, level, row, 1)
            vouched(jnp.logical_and(low, above), a_level, row, 1)

            @pl.when(jnp.logical_not(low))
            def _():
                send_owned(chip_at(met[0], row), 0)

            continue
        if place == 1:
            vouched(upper, level, 1, core)
            send_shared(chip_at(level, 1 - row))
            vouched(jnp.logical_and(met[0] > level, upper), met[0], 1, core)
            send_shared(chip_at(met[0], 1 - row))
        vouched(jnp.logical_and(above, upper), a_level, 1, core)
        send_shared(chip_at(a_level, 1 - row))

    send_owned(chip, 1 - core)
    vouched(low_upper, level, 1, 1)
    vouched(jnp.logical_and(low_upper, met[0] > level), met[0], 1, 1)
    for a_level in met[1:]:
        vouched(jnp.logical_and(low, a_level > level), a_level, row, 1)
        vouched(jnp.logical_and(low_upper, a_level > level), a_level, 1, 1)

    far_pairs = [(chip_at(a_level, 1 - row), chip_at(a_level, row)) for a_level in far_first]
    next_door = chip_at(level, 1 - row)
    across_chips = [to_chip for pair in far_pairs[:-1] for to_chip in pair]

    def send_all_owned(to_chips, last_chips, but=None):
        for to_chip in to_chips:
            send_owned(to_chip, 0)
        for to_chip in to_chips + last_chips:
            if to_chip is but:
                @pl.when(jnp.logical_not(shifts))
                def _():
                    send_owned(to_chip, 1)
            else:
                send_owned(to_chip, 1)

    inner = jnp.logical_or(level == levels // 2 - 1, level == levels // 2)

    @pl.when(inner)
    def _():
        send_all_owned(across_chips + [far_pairs[-1][0], next_door], [far_pairs[-1][1]])

    earlier[...] = (
        lax.broadcasted_iota(jnp.int32, (tokens, tokens), 1)
        < lax.broadcasted_iota(jnp.int32, (tokens, tokens), 0)
    ).astype(jnp.float32).astype(jnp.bfloat16)

    def settle_shared_sends():
        settle(shared.at[:, 0 : chips - 1, 0], send_sem.at[0])
        settle(seg_all.at[0 : chips - 1, 0], send_sem.at[0])

    lower = level < levels // 2
    shifts = jnp.logical_and(lower, row == 1)
    shifted_chip = chip_at(levels // 2, 0)
    outer = jnp.logical_not(inner)
    lower_outer = jnp.logical_and(lower, outer)

    @pl.when(outer)
    def _():
        send_all_owned([far_pairs[-1][0], next_door], [far_pairs[-1][1]])

    @pl.when(jnp.logical_not(lower_outer))
    def _():
        settle_shared_sends()

    @pl.when(jnp.logical_and(lower, inner))
    def _():
        for step in range(1, levels // 2):
            signal(go_sem, chip_at(level - step, row) * 2 + core)

    passes = jnp.logical_and(lower_outer, row == 0)

    @pl.when(jnp.logical_and(lower_outer, row == 1))
    def _():
        for j in range(own_heads):
            remote(
                staged.at[:, :, columns(shifted_chip * per_chip + own_head(j, 1))],
                passing.at[j], send_sem.at[1], relay_recv.at[2], me - 2,
            )

    @pl.when(lower_outer)
    def _():
        pl.semaphore_wait(go_sem, 1)

    @pl.when(outer)
    def _():
        send_all_owned(across_chips, [], across_chips[2])

    @pl.when(passes)
    def _():
        settle(passing, relay_recv.at[2])
        for j in range(own_heads):
            remote(
                passing.at[j], owned.at[j, :, me + 2],
                send_sem.at[1], recv_sem.at[2 + j], shifted_chip * 2 + 1,
            )

    settle(seg_all.at[0 : chips - 1, 0], seg_recv)
    relays = [remote(
        seg_all.at[:, core], seg_all.at[:, core], send_sem.at[1], relay_recv.at[0], partner
    )]
    settle(owned.at[0, :, 0 : 1 + own_heads], slot_sem)
    settle(shared.at[:, 0 : chips - 1, 0], recv_sem.at[0])
    relays.append(remote(
        shared.at[1:3, :, core], shared.at[1:3, :, core], send_sem.at[1], relay_recv.at[1], partner
    ))
    for copy in loads:
        copy.wait()
    relays[0].wait_recv()
    eye = (
        lax.broadcasted_iota(jnp.int32, (tok, tok), 0)
        == lax.broadcasted_iota(jnp.int32, (tok, tok), 1)
    ).astype(jnp.float32).astype(jnp.bfloat16)
    ids = lax.broadcasted_iota(jnp.int32, (LANES, tok), 0)
    for n in range(devices):
        flipped = (ids == seg_all[n // 2, n % 2]).astype(jnp.float32).astype(jnp.bfloat16)
        hot[n] = lax.dot_general(
            eye, flipped, CONTRACT_LAST, preferred_element_type=jnp.float32
        ).astype(jnp.bfloat16)
    all_hot = hot[...].reshape(tokens, LANES)
    before = jnp.dot(earlier[...], all_hot, preferred_element_type=jnp.float32)
    lane = lax.broadcasted_iota(jnp.int32, (1, LANES), 1)
    limit = jnp.zeros((1, LANES), jnp.int32)
    for r in range(requests):
        limit = jnp.where(lane == r, text_ref[0:1, r : r + 1], limit)
    inside = jnp.where(before < limit.astype(jnp.float32), all_hot.astype(jnp.float32), 0.0)
    text = jnp.dot(
        inside.astype(jnp.bfloat16), jnp.ones((LANES, LANES), jnp.bfloat16),
        preferred_element_type=jnp.float32,
    ) > 0.5
    query_gain, key_gain = query_gain_ref[...], key_gain_ref[...]
    spread = (chips, 2, tok, LANES)
    query_gains[...] = jnp.where(text, query_gain[0:1], query_gain[1:2]).reshape(spread)
    key_gains[...] = jnp.where(text, key_gain[0:1], key_gain[1:2]).reshape(spread)
    same = lax.dot_general(all_hot, all_hot, CONTRACT_LAST, preferred_element_type=jnp.float32)
    bias[...] = jnp.where(same > 0.5, 0.0, MASKED).reshape(chips, 2, tok, tokens)

    scale = 1.0 / math.sqrt(HEAD_DIM)

    def attention_weights(query_n, key_n, query_bias):
        scores = lax.dot_general(
            query_n, key_n, CONTRACT_LAST, preferred_element_type=jnp.float32
        ) * scale + query_bias
        grown = jnp.exp(scores - jnp.max(scores, axis=-1, keepdims=True))
        return (grown * (1.0 / jnp.sum(grown, axis=-1, keepdims=True))).astype(jnp.bfloat16)

    half = (tokens // 2, HEAD_DIM)
    full = (tokens, HEAD_DIM)
    query_n = normed(shared.at[0, :, core][...], query_gains.at[:, core][...]).reshape(half)
    relays[1].wait_recv()
    key_n = normed(shared[1], key_gains[...]).reshape(full)
    part_weights = attention_weights(
        query_n, key_n, bias.at[:, core][...].reshape(tokens // 2, tokens)
    )
    shared_out[...] = jnp.dot(
        part_weights, shared[2].reshape(full), preferred_element_type=jnp.float32
    ).astype(jnp.bfloat16).reshape(chips, tok, HEAD_DIM)

    number = lax.broadcasted_iota(jnp.int32, (LANES, LANES), 0).astype(jnp.float32)
    own_id = jnp.dot(hot[me], number.astype(jnp.bfloat16), preferred_element_type=jnp.float32)
    own_before = jnp.dot(
        earlier[pl.ds(pl.multiple_of(me * tok, tok), tok), :], all_hot,
        preferred_element_type=jnp.float32,
    )
    own_inside = jnp.where(
        own_before < limit.astype(jnp.float32), hot[me].astype(jnp.float32), 0.0
    )
    own_text = jnp.dot(
        own_inside.astype(jnp.bfloat16), jnp.ones((LANES, LANES), jnp.bfloat16),
        preferred_element_type=jnp.float32,
    )
    own_code = 2.0 * own_id + jnp.where(own_text > 0.5, 0.0, 1.0)
    for tile in range(hidden_ref.shape[1] // LANES):
        cols = slice(tile * LANES, (tile + 1) * LANES)
        total = jnp.zeros((tok, LANES), jnp.float32)
        for r in range(requests):
            pair = gate_ref[r, :, cols].astype(jnp.float32)
            for s in range(2):
                total = jnp.where(own_code == float(2 * r + s), pair[s : s + 1], total)
        gate_rows[tile] = total

    holder = lower_outer
    hold = jnp.logical_and(holder, low)
    lower_half = level < levels // 2
    lower_chips = list(range(chips // 2))
    upper_chips = list(range(chips // 2, chips))

    def send_shared_result(to_chip):
        remote(
            shared_out.at[to_chip], back.at[chip * per_chip],
            send_sem.at[1], recv_sem.at[1], to_chip * 2 + core,
        )

    def send_owned_result(j, to_chip):
        for a_core in range(2):
            remote(
                owned_out.at[j, to_chip, a_core], back.at[chip * per_chip + own_head(j, core)],
                send_sem.at[1], recv_sem.at[1], to_chip * 2 + a_core,
            )

    def send_results(to_chips, condition, send):
        for to_chip in to_chips:
            @pl.when(jnp.logical_and(condition, chip != to_chip))
            def _():
                send(to_chip)

    def send_shared_results(to_chips, condition):
        send_results(to_chips, condition, send_shared_result)

    def send_owned_results(j, to_chips, condition):
        send_results(to_chips, condition, functools.partial(send_owned_result, j))

    for j in range(own_heads):
        settle(owned.at[j, :, 0 : devices - 1], recv_sem.at[2 + j])
        if j == 0:
            @pl.when(jnp.logical_and(holder, core == 1))
            def _():
                signal(done_sem, partner)

            send_shared_results(lower_chips[2:], lower_half)
            send_shared_results(lower_chips[:2], chip >= 0)
            send_shared_results(upper_chips, jnp.logical_not(hold))
        flat = (devices, tok, LANES)
        key_n = normed(owned[j, 1], key_gains[...].reshape(flat)).reshape(full)
        value_all = owned[j, 2].reshape(full)
        head = chip * per_chip + own_head(j, core)
        for place, to_chips in enumerate((lower_chips, upper_chips)):
            chip_rows = pl.ds(place * (chips // 2), chips // 2)
            rows_in = owned[j, 0, place * chips : (place + 1) * chips]
            gain_rows = query_gains[chip_rows].reshape(chips, tok, LANES)
            query_n = normed(rows_in, gain_rows).reshape(half)
            bias_rows = bias[chip_rows].reshape(tokens // 2, tokens)
            owned_out[j, chip_rows] = jnp.dot(
                attention_weights(query_n, key_n, bias_rows), value_all,
                preferred_element_type=jnp.float32,
            ).astype(jnp.bfloat16).reshape(chips // 2, 2, tok, HEAD_DIM)
            if place == 0:
                send_owned_results(j, lower_chips[:2], chip >= 0)
                send_owned_results(j, lower_chips[2:], lower_half)
        send_owned_results(j, lower_chips[2:], jnp.logical_not(lower_half))
        send_owned_results(j, upper_chips, jnp.logical_not(hold))
        if j == 0:
            send_shared_results(lower_chips[2:], jnp.logical_not(lower_half))
        remote(
            owned_out.at[j, chip, 1 - core], back.at[head],
            send_sem.at[1], recv_sem.at[1], partner,
        )

    @pl.when(hold)
    def _():
        pl.semaphore_wait(done_sem, 1)
        for to_chip in upper_chips:
            send_shared_result(to_chip)
            for j in range(own_heads):
                send_owned_result(j, to_chip)

    def finish(head):
        cols = slice(head * HEAD_DIM, (head + 1) * HEAD_DIM)
        out_ref[:, cols] = (
            hidden_ref[:, cols].astype(jnp.float32)
            + gate_rows[head] * back[head].astype(jnp.float32)
        ).astype(jnp.bfloat16)

    @pl.when(lower_outer)
    def _():
        settle_shared_sends()

    @pl.when(passes)
    def _():
        settle(passing, send_sem.at[1])

    settle(seg_all.at[:, core], send_sem.at[1])
    settle(shared.at[1:3, :, core], send_sem.at[1])
    for j in range(own_heads):
        settle(owned.at[j, :, 0 : devices - 1], send_sem.at[1])
    results = back.at[0 : per_chip * (chips - 1) + own_heads]
    settle(results, send_sem.at[1])
    back[chip * per_chip] = shared_out[chip]
    for j in range(own_heads):
        back[chip * per_chip + own_head(j, core)] = owned_out.at[j, chip, core][...]
    settle(results, recv_sem.at[1])
    for head in range(chips * per_chip):
        finish(head)


def fused(
    hidden, queries, key_rows, values, query_gain, key_gain, gate_table, segment, text_count
):
    devices = lax.axis_size("seq")
    chips = devices // 2
    tok, width = hidden.shape
    heads = width // HEAD_DIM
    own_heads = heads // chips // 2
    tokens = devices * tok
    hbm = pl.BlockSpec(memory_space=pl.ANY)
    block = (tok, HEAD_DIM)
    dma = pltpu.SemaphoreType.DMA
    return pl.pallas_call(
        functools.partial(fused_kernel, devices),
        out_shape=jax.ShapeDtypeStruct((tok, width), jnp.bfloat16),
        in_specs=[hbm] * 9,
        out_specs=pl.BlockSpec(memory_space=pltpu.VMEM),
        scratch_shapes=[
            pltpu.VMEM((1, text_count.shape[0]), jnp.int32),
            pltpu.VMEM(hidden.shape, hidden.dtype),
            pltpu.VMEM(query_gain.shape, query_gain.dtype),
            pltpu.VMEM(key_gain.shape, key_gain.dtype),
            pltpu.VMEM(gate_table.shape, gate_table.dtype),
            pltpu.VMEM((3, tok, width), jnp.bfloat16),
            pltpu.VMEM((3, chips, 2) + block, jnp.bfloat16),
            pltpu.VMEM((own_heads, 3, devices) + block, jnp.bfloat16),
            pltpu.VMEM((own_heads, 3) + block, jnp.bfloat16),
            pltpu.VMEM((chips,) + block, jnp.bfloat16),
            pltpu.VMEM((own_heads, chips, 2) + block, jnp.bfloat16),
            pltpu.VMEM((heads,) + block, jnp.bfloat16),
            pltpu.VMEM((chips, 2, 1, tok), jnp.int32),
            pltpu.VMEM((devices, tok, LANES), jnp.bfloat16),
            pltpu.VMEM((tokens, tokens), jnp.bfloat16),
            pltpu.VMEM((chips, 2, tok, LANES), jnp.float32),
            pltpu.VMEM((chips, 2, tok, LANES), jnp.float32),
            pltpu.VMEM((chips, 2, tok, tokens), jnp.float32),
            pltpu.VMEM((heads, tok, LANES), jnp.float32),
            pltpu.SemaphoreType.REGULAR((devices,)),
            pltpu.SemaphoreType.REGULAR,
            pltpu.SemaphoreType.REGULAR,
            dma,
            dma,
            dma,
            dma,
            dma,
            dma((2,)),
            dma((2 + own_heads,)),
            dma((3,)),
        ],
        compiler_params=pltpu.CompilerParams(
            collective_id=0, has_side_effects=True, vmem_limit_bytes=16 * 1024 * 1024
        ),
    )(*(
        pltpu.with_memory_space_constraint(array, pltpu.HBM)
        for array in (
            segment.reshape(1, tok), queries, key_rows, values,
            text_count.reshape(1, -1), hidden, query_gain, key_gain, gate_table,
        )
    ))


def program(*arrays):
    devices = lax.axis_size("seq")
    tok, width = arrays[0].shape
    requests = arrays[-1].shape[0]
    whole_heads = devices % 8 == 0 and devices > 8 and (width // HEAD_DIM) % (devices // 2) == 0
    odd = whole_heads and width // HEAD_DIM // (devices // 2) % 2 == 1
    if odd and devices * tok <= 512 and requests <= LANES and tok % 16 == 0:
        return fused(*arrays)
    return per_device(*arrays)


def solution(mesh):
    return jax.shard_map(
        program,
        mesh=mesh,
        in_specs=(
            P(("groups", "seq"), None),
            P(("groups", "seq"), None),
            P(("groups", "seq"), None),
            P(("groups", "seq"), None),
            P(),
            P(),
            P("groups", None, None),
            P(("groups", "seq")),
            P("groups"),
        ),
        out_specs=P(("groups", "seq"), None),
        check_vma=False,
    )
```
